128 devices in a mesh: tm: 2 (over core), space: 64 (over z, y, x).
Axes of the slice: x: 4, y: 4, z: 4, core: 2. Of those that a mesh axis runs over, the one named last changes fastest.
Arguments:
- fine: bfloat16 [8, 256, 256, 256], P('tm', 'space'), may hold values from -6 to 6
- coarse: bfloat16 [8, 128, 128, 256], P('tm', 'space'), may hold values from -6 to 6
- w_query: bfloat16 [256, 256], replicated, may hold values from -24 to 24
- w_key: bfloat16 [256, 256], replicated, may hold values from -0.375 to 0.375
- w_value: bfloat16 [256, 256], replicated, may hold values from -0.375 to 0.375
- w_out: bfloat16 [256, 256], replicated, may hold values from -0.375 to 0.375
- conv_first: bfloat16 [3, 3, 256, 256], replicated, may hold values from -0.125 to 0.125
- conv_second: bfloat16 [3, 3, 256, 256], replicated, may hold values from -0.125 to 0.125
Outputs:
- joined: bfloat16 [8, 256, 256, 256], P('tm', 'space')
The draws below stay inside these ranges and needn't reach their ends.
All inputs are finite; a program needn't handle non-finite values.
Results may differ from the reference program's by a relative error of at most 0.009.
Values may be sent and summed in bfloat16 or wider, within the bound.
A program may use at most 128 MiB of HBM per device.

```python
import jax
import jax.numpy as jnp
from jax import lax

C = 256
HEADS = 8
W = 256
FRAMES = 8
H = 256


def draw_w_query(key, part):
    base = jax.random.normal(jax.random.fold_in(key, 11), (C, C), jnp.float32) / jnp.sqrt(jnp.float32(C))
    base = jnp.clip(base, -6.0 / jnp.sqrt(jnp.float32(C)), 6.0 / jnp.sqrt(jnp.float32(C)))
    logs = jax.random.uniform(jax.random.fold_in(key, 12), (HEADS,), jnp.float32, jnp.log(0.5), jnp.log(3.0))
    columns = jnp.repeat(jnp.exp(logs), C // HEADS)
    return (base * columns[None, :]).astype(jnp.bfloat16)


def shard_levels(own_key, extent, split, least, high):
    loudness, own = 1.0, jax.random.fold_in(own_key, 6)
    for axis_at, blocks in split:
        heights = jnp.exp(jax.random.uniform(jax.random.fold_in(own, axis_at), (blocks,), jnp.float32, least / len(split), high / len(split)))
        loudness = loudness * jnp.repeat(heights, extent[axis_at] // blocks).reshape([-1 if axis == axis_at else 1 for axis in range(len(extent))])
    return loudness


def scatter_about(own_key, extent, deviation, reach, shards=(), kind=jnp.bfloat16):
    entries = jax.random.normal(own_key, extent, jnp.float32) * deviation
    if len(shards) > 0:
        entries = shard_levels(own_key, extent, shards, -0.22, 0.18) * entries
    return jnp.clip(entries, min=-reach, max=reach).astype(kind)


def setup_inputs(seed: int = 0) -> dict:
    arg_keys = jax.random.split(jax.random.key(seed), 9)
    return {
        "fine": scatter_about(arg_keys[0], (FRAMES, H, W, C), 1.0, 6.0, ((0, 2), (1, 64))),
        "coarse": scatter_about(arg_keys[1], (FRAMES, H // 2, W // 2, C), 1.0, 6.0, ((0, 2), (1, 64))),
        "w_query": draw_w_query(jax.random.fold_in(arg_keys[8], 71), 0),
        "w_key": scatter_about(arg_keys[3], (C, C), C ** -0.5, 0.375),
        "w_value": scatter_about(arg_keys[4], (C, C), C ** -0.5, 0.375),
        "w_out": scatter_about(arg_keys[5], (C, C), C ** -0.5, 0.375),
        "conv_first": scatter_about(arg_keys[6], (3, 3, C, C), (9 * C) ** -0.5, 0.125),
        "conv_second": scatter_about(arg_keys[7], (3, 3, C, C), (9 * C) ** -0.5, 0.125),
    }


def encode(frame_ids, width):
    half = width // 2
    index = jnp.arange(half, dtype=jnp.float32)
    inverse = jnp.exp(-jnp.log(10000.0) * 2.0 * index / width)
    angles = frame_ids.astype(jnp.float32)[:, None] * inverse[None, :]
    return jnp.concatenate([jnp.sin(angles), jnp.cos(angles)], axis=1)

def normalize(features, frame_ids):
    width = features.shape[-1]
    hidden = features.astype(jnp.float32) + encode(frame_ids, width)[:, None, None, :]
    center = hidden - lax.optimization_barrier(jnp.mean(hidden, axis=-1, keepdims=True))
    spread = lax.optimization_barrier(jnp.mean(center * center, axis=-1, keepdims=True))
    return (center * lax.rsqrt(spread + 1e-05)).astype(jnp.bfloat16)

def project(normed, weight):
    shape = normed.shape
    flat = normed.reshape(-1, shape[-1])
    return jnp.dot(flat, weight, preferred_element_type=jnp.float32).astype(jnp.bfloat16).reshape(shape)

def attend(query, key, value):
    frames, rows, cols, width = query.shape
    depth = width // HEADS
    query_heads = query.reshape(frames, rows * cols, HEADS, depth).astype(jnp.float32)
    key_heads = key.reshape(key.shape[0], rows * cols, HEADS, depth).astype(jnp.float32)
    value_heads = value.reshape(value.shape[0], rows * cols, HEADS, depth).astype(jnp.float32)
    scores = jnp.einsum('qphd,kphd->qkhp', query_heads, key_heads) / jnp.sqrt(jnp.float32(depth))
    weights = jax.nn.softmax(scores, axis=1).astype(jnp.bfloat16)
    attended = jnp.einsum('qkhp,kphd->qphd', weights.astype(jnp.float32), value_heads)
    return attended.astype(jnp.bfloat16).reshape(frames, rows, cols, width)

def convolve(features, weight):
    return lax.conv_general_dilated(features.astype(jnp.float32), weight.astype(jnp.float32), (1, 1), 'SAME', dimension_numbers=('NHWC', 'HWIO', 'NHWC'), precision=lax.Precision.HIGHEST)

def double(extended, axis):
    count = extended.shape[axis] - 2
    middle = lax.slice_in_dim(extended, 1, count + 1, axis=axis)
    before = lax.slice_in_dim(extended, 0, count, axis=axis)
    after = lax.slice_in_dim(extended, 2, count + 2, axis=axis)
    even = 0.75 * middle + 0.25 * before
    odd = 0.75 * middle + 0.25 * after
    stacked = jnp.stack([even, odd], axis=axis + 1)
    shape = list(middle.shape)
    shape[axis] = 2 * count
    return stacked.reshape(shape)

def upsample(coarse):
    values = coarse.astype(jnp.float32)
    extended = jnp.pad(values, ((0, 0), (1, 1), (0, 0), (0, 0)), mode='edge')
    rows_done = double(extended, 1)
    extended = jnp.pad(rows_done, ((0, 0), (0, 0), (1, 1), (0, 0)), mode='edge')
    return double(extended, 2)

def reference(fine, coarse, w_query, w_key, w_value, w_out, conv_first, conv_second):
    frame_ids = jnp.arange(fine.shape[0], dtype=jnp.int32)
    normed = normalize(fine, frame_ids)
    query = project(normed, w_query)
    key = project(normed, w_key)
    value = project(normed, w_value)
    attended = attend(query, key, value)
    shape = fine.shape
    branch = jnp.dot(attended.reshape(-1, shape[-1]), w_out, preferred_element_type=jnp.float32).reshape(shape)
    moved = (fine.astype(jnp.float32) + branch).astype(jnp.bfloat16)
    first = convolve(jax.nn.relu(moved), conv_first).astype(jnp.bfloat16)
    second = convolve(jax.nn.relu(first), conv_second)
    up = upsample(coarse)
    return (up + moved.astype(jnp.float32) + second).astype(jnp.bfloat16)
```

```python
import numpy as np
import jax
import jax.numpy as jnp
from jax import lax
from jax.experimental import pallas as pl
from jax.experimental.pallas import tpu as pltpu
from jax.sharding import PartitionSpec as P

HEADS = 8
C = 256
W = 256
FL = 4
RL = 4
BF = jnp.bfloat16
F32 = jnp.float32
MESH = pl.DeviceIdType.MESH


def tables():
    at = np.arange(256)
    col_of = (at % 16) * 16 + at // 16
    columns = np.zeros((256, 256), np.float32)
    columns[at, col_of] = 1.0
    channel = np.zeros((256, 256), np.float32)
    channel[at, (at % 32) * 8 + at // 32] = 1.0
    same = (at[:, None] // 128 == at[None, :] // 128) & (at[:, None] % 8 == at[None, :] % 8)
    heads = same.astype(np.float32)
    widen = np.zeros((256, 128), np.float32)
    for col in range(256):
        half = col // 2
        other = max(half - 1, 0) if col % 2 == 0 else min(half + 1, 127)
        widen[col, half] += 0.75
        widen[col, other] += 0.25
    widen = widen[col_of]
    none = np.zeros_like(widen)

    def pair(first, second):
        return np.concatenate([first * widen, second * widen], axis=1)

    stack = [columns, channel, channel.T, heads, pair(0.75, 0), pair(0.75, 0.25), pair(0.25, 0.75), pair(0, 0.75), pair(0.25, 0), pair(0, 0.25)]
    return np.stack(stack).astype(jnp.bfloat16)


def positions():
    half = C // 2
    inverse = np.exp(-np.log(10000.0) * 2.0 * np.arange(half) / C)
    angles = np.arange(8)[:, None] * inverse[None, :]
    return np.concatenate([np.sin(angles), np.cos(angles)], axis=1).astype(np.float32)[:, None, :]


def taps(ref, lead, first, rows):
    parts = []
    for dy in range(3):
        for dx in range(3):
            parts.append(ref[lead, first + dy : first + dy + rows, 16 * dx : 16 * dx + 256, :].reshape(rows * 256, C))
    return jnp.concatenate(parts, axis=1)


def pads(ref, lead, row):
    index = lax.broadcasted_iota(jnp.int32, (16, C), 0)
    last = ref[lead, row, 256:272, :].astype(F32)
    before = jnp.where(index == 0, 0.0, pltpu.roll(last, 1, axis=0))
    ref[lead, row, 0:16, :] = before.astype(BF)
    leading = ref[lead, row, 16:32, :].astype(F32)
    after = jnp.where(index == 15, 0.0, pltpu.roll(leading, 15, axis=0))
    ref[lead, row, 272:288, :] = after.astype(BF)


def kernel(
    spaces,
    fine_hbm, coarse_hbm, wq_hbm, wk_hbm, wv_hbm, wo_hbm, c1_hbm, c2_hbm, mats_hbm, pos_hbm,
    out_hbm,
    fin, cb, raw, mats, pos, cw1, cw2,
    wqp, wkv, wop, nbuf, fp, qs, kb, vb, att, xp, yp, acc, ob, psend, precv,
    load_sem, row_sem, nsend, nrecv, xsend, xrecv, tsend, trecv, out_sem,
):
    t = lax.axis_index("tm")
    s = lax.axis_index("space")
    has_up = s > 0
    has_down = s < spaces - 1

    def row_load(r):
        return pltpu.make_async_copy(fine_hbm.at[:, r], fin.at[:, r], row_sem.at[r])

    loads = [
        pltpu.make_async_copy(mats_hbm, mats, load_sem.at[0]),
        pltpu.make_async_copy(pos_hbm, pos, load_sem.at[1]),
        pltpu.make_async_copy(wq_hbm, raw.at[0], load_sem.at[2]),
        pltpu.make_async_copy(wk_hbm, raw.at[1], load_sem.at[3]),
        pltpu.make_async_copy(wv_hbm, raw.at[2], load_sem.at[4]),
        pltpu.make_async_copy(wo_hbm, raw.at[3], load_sem.at[5]),
        pltpu.make_async_copy(coarse_hbm, cb, load_sem.at[6]),
        pltpu.make_async_copy(c1_hbm, cw1, load_sem.at[7]),
        pltpu.make_async_copy(c2_hbm, cw2, load_sem.at[8]),
    ]
    loads[0].start()
    loads[1].start()
    row_load(0).start()
    row_load(3).start()
    for copy in loads[2:6]:
        copy.start()
    row_load(1).start()
    row_load(2).start()
    for copy in loads[6:]:
        copy.start()

    barrier = pltpu.get_barrier_semaphore()
    pl.semaphore_signal(barrier, inc=1, device_id=(1 - t, s), device_id_type=MESH)

    @pl.when(has_up)
    def _():
        pl.semaphore_signal(barrier, inc=1, device_id=(t, s - 1), device_id_type=MESH)

    @pl.when(has_down)
    def _():
        pl.semaphore_signal(barrier, inc=1, device_id=(t, s + 1), device_id_type=MESH)

    zero_row = jnp.zeros((FL, 288, C), BF)
    yp[:, 0] = zero_row
    yp[:, 5] = zero_row

    @pl.when(jnp.logical_not(has_up))
    def _():
        xp[:, 0] = zero_row

    @pl.when(jnp.logical_not(has_down))
    def _():
        xp[:, 5] = zero_row

    loads[0].wait()
    loads[1].wait()
    for copy in loads[2:6]:
        copy.wait()
    wqp[...] = jnp.dot(raw[0], mats[1], preferred_element_type=F32).astype(BF)
    wkv[:, 0:256] = jnp.dot(raw[1], mats[1], preferred_element_type=F32).astype(BF)
    wkv[:, 256:512] = jnp.dot(raw[2], mats[1], preferred_element_type=F32).astype(BF)
    wop[...] = jnp.dot(mats[2], raw[3], preferred_element_type=F32).astype(BF)

    pl.semaphore_wait(barrier, 1 + has_up.astype(jnp.int32) + has_down.astype(jnp.int32))

    def norm_copy(f, r):
        return pltpu.make_async_remote_copy(
            src_ref=nbuf.at[f, r], dst_ref=nbuf.at[f + FL, r],
            send_sem=nsend.at[f, r], recv_sem=nrecv.at[f, r],
            device_id=(1 - t, s), device_id_type=MESH)

    def normalize(rows):
        for r in rows:
            row_load(r).wait()

        def step(f, carry):
            for r in rows:
                moved = jnp.dot(mats[0], fin[f, r], preferred_element_type=F32)
                fp[f, r] = moved.astype(BF)
                hidden = moved + pos[t * FL + f]
                center = hidden - jnp.mean(hidden, axis=-1, keepdims=True)
                spread = jnp.mean(center * center, axis=-1, keepdims=True)
                nbuf[f, r] = (center * lax.rsqrt(spread + 1e-05)).astype(BF)
            for r in rows:
                norm_copy(f, r).start()
            return carry

        lax.fori_loop(0, FL, step, 0)

    def edge_copy(a, up):
        row, slot, to = (1, 5, s - 1) if up else (4, 0, s + 1)
        side = 0 if up else 1
        return pltpu.make_async_remote_copy(
            src_ref=xp.at[a, row, pl.ds(16, 256)], dst_ref=xp.at[a, slot, pl.ds(16, 256)],
            send_sem=xsend.at[side, a], recv_sem=xrecv.at[side, a],
            device_id=(t, to), device_id_type=MESH)

    def part_copy(a, up):
        side = 0 if up else 1
        to = s - 1 if up else s + 1
        return pltpu.make_async_remote_copy(
            src_ref=psend.at[side, a], dst_ref=precv.at[side, a],
            send_sem=tsend.at[side, a], recv_sem=trecv.at[side, a],
            device_id=(t, to), device_id_type=MESH)

    factor = float(np.log2(np.e) / np.sqrt(32.0))

    def keys(rows):
        def step(b, carry):
            for i, r in enumerate(rows):
                both = jnp.dot(nbuf[b, r], wkv[...], preferred_element_type=F32)
                kb[i, b] = both[:, 0:256].astype(BF)
                vb[i, b] = both[:, 256:512].astype(BF)
            return carry

        lax.fori_loop(0, FL, step, 0)
        for r in rows:
            for f in range(FL):
                norm_copy(f, r).wait_recv()
        lax.fori_loop(FL, 2 * FL, step, 0)

    def attend(rows, edges):
        def step(a, carry):
            for i, r in enumerate(rows):
                query = jnp.dot(nbuf[a, r], wqp[...], preferred_element_type=F32) * factor
                qs[i] = query.astype(BF)
                for blk in range(4):
                    px = slice(64 * blk, 64 * blk + 64)
                    q = qs[i, px]
                    lhs = []
                    for pair in range(4):
                        halves = []
                        for b in (2 * pair, 2 * pair + 1):
                            product = q * kb[i, b, px]
                            halves.append(product[:, 0:128] + product[:, 128:256])
                        lhs.append(jnp.concatenate(halves, axis=1))
                    both = jnp.dot(jnp.concatenate(lhs, axis=0), mats[3], preferred_element_type=F32)
                    scores = []
                    for b in range(8):
                        at = 64 * (b // 2)
                        scores.append(both[at : at + 64, 128 * (b % 2) : 128 * (b % 2) + 128])
                    largest = scores[0]
                    for entry in scores[1:]:
                        largest = jnp.maximum(largest, entry)
                    powers = [jnp.exp2(entry - largest) for entry in scores]
                    total = powers[0]
                    for entry in powers[1:]:
                        total = total + entry
                    inverse = 1.0 / total
                    low, high = [], []
                    for b in range(8):
                        weight = powers[b].astype(BF)
                        value = vb[i, b, px]
                        low.append(weight * value[:, 0:128])
                        high.append(weight * value[:, 128:256])
                    while len(low) > 1:
                        low = [low[j] + low[j + 1] for j in range(0, len(low), 2)]
                        high = [high[j] + high[j + 1] for j in range(0, len(high), 2)]
                    att[i, px, 0:128] = (low[0].astype(F32) * inverse).astype(BF)
                    att[i, px, 128:256] = (high[0].astype(F32) * inverse).astype(BF)
                branch = jnp.dot(att[i], wop[...], preferred_element_type=F32)
                moved = (fp[a, r].astype(F32) + branch).astype(BF)
                fp[a, r] = moved
                xp[a, r + 1, 16:272, :] = jnp.maximum(moved, jnp.zeros_like(moved))
            if edges:
                @pl.when(has_up)
                def _():
                    edge_copy(a, True).start()

                @pl.when(has_down)
                def _():
                    edge_copy(a, False).start()
            return carry

        lax.fori_loop(0, FL, step, 0)

    normalize((0, 3))
    normalize((1, 2))
    keys((0, 3))
    attend((0, 3), True)
    keys((1, 2))
    attend((1, 2), False)

    for copy in loads[6:]:
        copy.wait()

    def first_step(a, carry):
        for r in range(1, 5):
            pads(xp, a, r)

        @pl.when(has_up)
        def _():
            edge_copy(a, False).wait_recv()
            pads(xp, a, 0)

        @pl.when(has_down)
        def _():
            edge_copy(a, True).wait_recv()
            pads(xp, a, 5)

        weight = cw1[...].reshape(9 * C, C)
        for y in (0, 2):
            result = jnp.dot(taps(xp, a, y, 2), weight, preferred_element_type=F32)
            result = jnp.maximum(result, 0.0).astype(BF)
            yp[a, 1 + y : 3 + y, 16:272, :] = result.reshape(2, 256, C)
        for r in range(1, 5):
            pads(yp, a, r)
        near = cb[a].reshape(256, C)
        for side, row, dy in ((0, 1, 2), (1, 4, 0)):
            lhs = jnp.concatenate([yp[a, row, 16 * dx : 16 * dx + 256, :] for dx in range(3)], axis=1)
            part = jnp.dot(lhs, cw2[dy].reshape(3 * C, C), preferred_element_type=F32)
            part = part + jnp.dot(mats[8 + side], near, preferred_element_type=F32)
            psend[side, a] = part.astype(BF)

        @pl.when(has_up)
        def _():
            part_copy(a, True).start()

        @pl.when(has_down)
        def _():
            part_copy(a, False).start()

        return carry

    lax.fori_loop(0, FL, first_step, 0)

    def second_step(a, carry):
        weight = cw2[...].reshape(9 * C, C)
        near = cb[a].reshape(256, C)
        for y in (0, 2):
            result = jnp.dot(taps(yp, a, y, 2), weight, preferred_element_type=F32)
            for k in range(2):
                row = y + k
                up = jnp.dot(mats[4 + row], near, preferred_element_type=F32)
                value = result[256 * k : 256 * k + 256] + up + fp[a, row].astype(F32)
                if row in (1, 2):
                    ob[a, row] = value.astype(BF)
                else:
                    acc[a, row // 3] = value
        return carry

    lax.fori_loop(0, FL, second_step, 0)

    def edge_part(a, side):
        near = cb[a].reshape(256, C)
        precv[1 - side, a] = jnp.dot(mats[8 + side], near, preferred_element_type=F32).astype(BF)

    def last_step(a, carry):
        @pl.when(has_up)
        def _():
            part_copy(a, False).wait_recv()

        @pl.when(jnp.logical_not(has_up))
        def _():
            edge_part(a, 0)

        @pl.when(has_down)
        def _():
            part_copy(a, True).wait_recv()

        @pl.when(jnp.logical_not(has_down))
        def _():
            edge_part(a, 1)

        ob[a, 0] = (acc[a, 0] + precv[1, a].astype(F32)).astype(BF)
        ob[a, 3] = (acc[a, 1] + precv[0, a].astype(F32)).astype(BF)
        pltpu.make_async_copy(ob.at[a], out_hbm.at[a], out_sem.at[a]).start()
        return carry

    lax.fori_loop(0, FL, last_step, 0)

    def drain(a, carry):
        pltpu.make_async_copy(ob.at[a], out_hbm.at[a], out_sem.at[a]).wait()
        for r in range(RL):
            norm_copy(a, r).wait_send()

        @pl.when(has_up)
        def _():
            edge_copy(a, True).wait_send()
            part_copy(a, True).wait_send()

        @pl.when(has_down)
        def _():
            edge_copy(a, False).wait_send()
            part_copy(a, False).wait_send()

        return carry

    lax.fori_loop(0, FL, drain, 0)


def restore_kernel(mat, x, o):
    o[0, 0] = jnp.dot(mat[...], x[0, 0], preferred_element_type=F32).astype(BF)


def solution(mesh):
    spaces = mesh.shape["space"]
    constants = tables()
    place = positions()

    def local(fine, coarse, w_query, w_key, w_value, w_out, conv_first, conv_second):
        anywhere = pl.BlockSpec(memory_space=pl.ANY)
        dma = pltpu.SemaphoreType.DMA
        shape = (FL, RL, W, C)
        mats = jnp.asarray(constants)
        moved = pl.pallas_call(
            lambda *refs: kernel(spaces, *refs),
            out_shape=jax.ShapeDtypeStruct(shape, BF),
            in_specs=[anywhere] * 10,
            out_specs=anywhere,
            scratch_shapes=[
                pltpu.VMEM(shape, BF),
                pltpu.VMEM((FL, 2, 128, C), BF),
                pltpu.VMEM((4, C, C), BF),
                pltpu.VMEM((10, 256, 256), BF),
                pltpu.VMEM((8, 1, C), F32),
                pltpu.VMEM((3, 3, C, C), BF),
                pltpu.VMEM((3, 3, C, C), BF),
                pltpu.VMEM((C, C), BF),
                pltpu.VMEM((C, 2 * C), BF),
                pltpu.VMEM((C, C), BF),
                pltpu.VMEM((2 * FL, RL, W, C), BF),
                pltpu.VMEM(shape, BF),
                pltpu.VMEM((2, W, C), BF),
                pltpu.VMEM((2, 2 * FL, W, C), BF),
                pltpu.VMEM((2, 2 * FL, W, C), BF),
                pltpu.VMEM((2, W, C), BF),
                pltpu.VMEM((FL, RL + 2, W + 32, C), BF),
                pltpu.VMEM((FL, RL + 2, W + 32, C), BF),
                pltpu.VMEM((FL, 2, W, C), F32),
                pltpu.VMEM(shape, BF),
                pltpu.VMEM((2, FL, W, C), BF),
                pltpu.VMEM((2, FL, W, C), BF),
                dma((9,)),
                dma((RL,)),
                dma((FL, RL)),
                dma((FL, RL)),
                dma((2, FL)),
                dma((2, FL)),
                dma((2, FL)),
                dma((2, FL)),
                dma((FL,)),
            ],
            compiler_params=pltpu.CompilerParams(
                collective_id=0, has_side_effects=True, vmem_limit_bytes=60 * 1024 * 1024),
            name="fused",
        )(fine, coarse, w_query, w_key, w_value, w_out, conv_first, conv_second, mats, jnp.asarray(place))
        block = pl.BlockSpec((1, 1, W, C), lambda i, j: (i, j, 0, 0))
        return pl.pallas_call(
            restore_kernel,
            grid=(FL, RL),
            out_shape=jax.ShapeDtypeStruct(shape, BF),
            in_specs=[pl.BlockSpec((None, 256, 256), lambda i, j: (0, 0, 0)), block],
            out_specs=block,
            name="restore",
        )(mats, moved)

    return jax.shard_map(
        local,
        mesh=mesh,
        in_specs=(P("tm", "space", None, None), P("tm", "space", None, None), P(), P(), P(), P(), P(), P()),
        out_specs=P("tm", "space", None, None),
        check_vma=False,
    )
```

```python
import numpy as np
import jax
import jax.numpy as jnp
from jax import lax
from jax.experimental import pallas as pl
from jax.experimental.pallas import tpu as pltpu
from jax.sharding import PartitionSpec as P

HEADS = 8
C = 256
W = 256
FL = 4
RL = 4
BF = jnp.bfloat16
F32 = jnp.float32
MESH = pl.DeviceIdType.MESH


def tables():
    at = np.arange(256)
    col_of = (at % 16) * 16 + at // 16
    columns = np.zeros((256, 256), np.float32)
    columns[at, col_of] = 1.0
    channel = np.zeros((256, 256), np.float32)
    channel[at, (at % 32) * 8 + at // 32] = 1.0
    same = (at[:, None] // 128 == at[None, :] // 128) & (at[:, None] % 8 == at[None, :] % 8)
    heads = same.astype(np.float32)
    widen = np.zeros((256, 128), np.float32)
    for col in range(256):
        half = col // 2
        other = max(half - 1, 0) if col % 2 == 0 else min(half + 1, 127)
        widen[col, half] += 0.75
        widen[col, other] += 0.25
    widen = widen[col_of]
    none = np.zeros_like(widen)

    def pair(first, second):
        return np.concatenate([first * widen, second * widen], axis=1)

    stack = [columns, channel, channel.T, heads, pair(0.75, 0), pair(0.75, 0.25), pair(0.25, 0.75), pair(0, 0.75), pair(0.25, 0), pair(0, 0.25)]
    return np.stack(stack).astype(jnp.bfloat16)


def positions():
    half = C // 2
    inverse = np.exp(-np.log(10000.0) * 2.0 * np.arange(half) / C)
    angles = np.arange(8)[:, None] * inverse[None, :]
    return np.concatenate([np.sin(angles), np.cos(angles)], axis=1).astype(np.float32)[:, None, :]


def taps(ref, lead, first, rows):
    parts = []
    for dy in range(3):
        for dx in range(3):
            parts.append(ref[lead, first + dy : first + dy + rows, 16 * dx : 16 * dx + 256, :].reshape(rows * 256, C))
    return jnp.concatenate(parts, axis=1)


def pads(ref, lead, row):
    index = lax.broadcasted_iota(jnp.int32, (16, C), 0)
    last = ref[lead, row, 256:272, :].astype(F32)
    before = jnp.where(index == 0, 0.0, pltpu.roll(last, 1, axis=0))
    ref[lead, row, 0:16, :] = before.astype(BF)
    leading = ref[lead, row, 16:32, :].astype(F32)
    after = jnp.where(index == 15, 0.0, pltpu.roll(leading, 15, axis=0))
    ref[lead, row, 272:288, :] = after.astype(BF)


def kernel(
    spaces,
    fine_hbm, coarse_hbm, wq_hbm, wk_hbm, wv_hbm, wo_hbm, c1_hbm, c2_hbm, mats_hbm, pos_hbm,
    ob,
    fin, cb, raw, mats, pos, cw1, cw2,
    wqp, wkv, wop, nbuf, fp, qs, kb, vb, att, xp, yp, acc, psend, precv,
    load_sem, row_sem, nsend, nrecv, xsend, xrecv, tsend, trecv,
):
    t = lax.axis_index("tm")
    s = lax.axis_index("space")
    has_up = s > 0
    has_down = s < spaces - 1

    def row_load(r):
        return pltpu.make_async_copy(fine_hbm.at[:, r], fin.at[:, r], row_sem.at[r])

    loads = [
        pltpu.make_async_copy(mats_hbm, mats, load_sem.at[0]),
        pltpu.make_async_copy(pos_hbm, pos, load_sem.at[1]),
        pltpu.make_async_copy(wq_hbm, raw.at[0], load_sem.at[2]),
        pltpu.make_async_copy(wk_hbm, raw.at[1], load_sem.at[3]),
        pltpu.make_async_copy(wv_hbm, raw.at[2], load_sem.at[4]),
        pltpu.make_async_copy(wo_hbm, raw.at[3], load_sem.at[5]),
        pltpu.make_async_copy(coarse_hbm, cb, load_sem.at[6]),
        pltpu.make_async_copy(c1_hbm, cw1, load_sem.at[7]),
        pltpu.make_async_copy(c2_hbm, cw2, load_sem.at[8]),
    ]
    loads[0].start()
    loads[1].start()
    row_load(0).start()
    row_load(3).start()
    for copy in loads[2:6]:
        copy.start()
    row_load(1).start()
    row_load(2).start()
    for copy in loads[6:]:
        copy.start()

    barrier = pltpu.get_barrier_semaphore()
    pl.semaphore_signal(barrier, inc=1, device_id=(1 - t, s), device_id_type=MESH)

    @pl.when(has_up)
    def _():
        pl.semaphore_signal(barrier, inc=1, device_id=(t, s - 1), device_id_type=MESH)

    @pl.when(has_down)
    def _():
        pl.semaphore_signal(barrier, inc=1, device_id=(t, s + 1), device_id_type=MESH)

    zero_row = jnp.zeros((FL, 288, C), BF)
    yp[:, 0] = zero_row
    yp[:, 5] = zero_row

    @pl.when(jnp.logical_not(has_up))
    def _():
        xp[:, 0] = zero_row

    @pl.when(jnp.logical_not(has_down))
    def _():
        xp[:, 5] = zero_row

    with jax.named_scope("load_wait"):
        loads[0].wait()
        loads[1].wait()
        for copy in loads[2:6]:
            copy.wait()
    wqp[...] = jnp.dot(raw[0], mats[1], preferred_element_type=F32).astype(BF)
    wkv[:, 0:256] = jnp.dot(raw[1], mats[1], preferred_element_type=F32).astype(BF)
    wkv[:, 256:512] = jnp.dot(raw[2], mats[1], preferred_element_type=F32).astype(BF)
    wop[...] = jnp.dot(mats[2], raw[3], preferred_element_type=F32).astype(BF)

    with jax.named_scope("barrier"):
        pl.semaphore_wait(barrier, 1 + has_up.astype(jnp.int32) + has_down.astype(jnp.int32))

    def norm_copy(f, r):
        return pltpu.make_async_remote_copy(
            src_ref=nbuf.at[f, r], dst_ref=nbuf.at[f + FL, r],
            send_sem=nsend.at[f, r], recv_sem=nrecv.at[f, r],
            device_id=(1 - t, s), device_id_type=MESH)

    def normalize(rows):
        for r in rows:
            row_load(r).wait()

        def step(pair, carry):
            units = [(2 * pair + k, r) for k in range(2) for r in rows]
            placed = [jnp.dot(mats[0], fin[f, r], preferred_element_type=F32) for f, r in units]
            for (f, r), moved in zip(units, placed):
                fp[f, r] = moved.astype(BF)
                hidden = moved + pos[t * FL + f]
                center = hidden - jnp.mean(hidden, axis=-1, keepdims=True)
                spread = jnp.mean(center * center, axis=-1, keepdims=True)
                nbuf[f, r] = (center * lax.rsqrt(spread + 1e-05)).astype(BF)
            for f, r in units:
                norm_copy(f, r).start()
            return carry

        lax.fori_loop(0, FL // 2, step, 0)

    def edge_copy(a, up):
        row, slot, to = (1, 5, s - 1) if up else (4, 0, s + 1)
        side = 0 if up else 1
        return pltpu.make_async_remote_copy(
            src_ref=xp.at[a, row, pl.ds(16, 256)], dst_ref=xp.at[a, slot, pl.ds(16, 256)],
            send_sem=xsend.at[side, a], recv_sem=xrecv.at[side, a],
            device_id=(t, to), device_id_type=MESH)

    def part_copy(a, up):
        side = 0 if up else 1
        to = s - 1 if up else s + 1
        return pltpu.make_async_remote_copy(
            src_ref=psend.at[side, a], dst_ref=precv.at[side, a],
            send_sem=tsend.at[side, a], recv_sem=trecv.at[side, a],
            device_id=(t, to), device_id_type=MESH)

    factor = float(np.log2(np.e) / np.sqrt(32.0))

    def keys(rows):
        def step(own, pair, carry):
            frames = [2 * pair + k for k in range(2)]
            results, queries = [], []
            for b in frames:
                stacked = jnp.concatenate([nbuf[b, r] for r in rows], axis=0)
                results.append(jnp.dot(stacked, wkv[...], preferred_element_type=F32))
                if own:
                    queries.append(jnp.dot(stacked, wqp[...], preferred_element_type=F32))
            for b, both in zip(frames, results):
                for i in range(2):
                    kb[i, b] = both[256 * i : 256 * i + 256, 0:256].astype(BF)
                    vb[i, b] = both[256 * i : 256 * i + 256, 256:512].astype(BF)
            for b, query in zip(frames, queries):
                for i in range(2):
                    qs[i, b] = (query[256 * i : 256 * i + 256] * factor).astype(BF)
            return carry

        lax.fori_loop(0, FL // 2, lambda i, c: step(True, i, c), 0)
        with jax.named_scope("norm_wait"):
            for r in rows:
                for f in range(FL):
                    norm_copy(f, r).wait_recv()
        lax.fori_loop(FL // 2, FL, lambda i, c: step(False, i, c), 0)

    def attend(rows, edges):
        def step(a, carry):
            for i, r in enumerate(rows):
                for blk in range(4):
                    px = slice(64 * blk, 64 * blk + 64)
                    q = qs[i, a, px]
                    lhs = []
                    for pair in range(4):
                        halves = []
                        for b in (2 * pair, 2 * pair + 1):
                            product = q * kb[i, b, px]
                            halves.append(product[:, 0:128] + product[:, 128:256])
                        lhs.append(jnp.concatenate(halves, axis=1))
                    both = jnp.dot(jnp.concatenate(lhs, axis=0), mats[3], preferred_element_type=F32)
                    scores = []
                    for b in range(8):
                        at = 64 * (b // 2)
                        scores.append(both[at : at + 64, 128 * (b % 2) : 128 * (b % 2) + 128])
                    largest = scores[0]
                    for entry in scores[1:]:
                        largest = jnp.maximum(largest, entry)
                    powers = [jnp.exp2(entry - largest) for entry in scores]
                    total = powers[0]
                    for entry in powers[1:]:
                        total = total + entry
                    inverse = 1.0 / total
                    low, high = [], []
                    for b in range(8):
                        weight = powers[b].astype(BF)
                        value = vb[i, b, px]
                        low.append(weight * value[:, 0:128])
                        high.append(weight * value[:, 128:256])
                    while len(low) > 1:
                        low = [low[j] + low[j + 1] for j in range(0, len(low), 2)]
                        high = [high[j] + high[j + 1] for j in range(0, len(high), 2)]
                    att[i, px, 0:128] = (low[0].astype(F32) * inverse).astype(BF)
                    att[i, px, 128:256] = (high[0].astype(F32) * inverse).astype(BF)
                branch = jnp.dot(att[i], wop[...], preferred_element_type=F32)
                moved = (fp[a, r].astype(F32) + branch).astype(BF)
                fp[a, r] = moved
                xp[a, r + 1, 16:272, :] = jnp.maximum(moved, jnp.zeros_like(moved))
            if edges:
                @pl.when(has_up)
                def _():
                    edge_copy(a, True).start()

                @pl.when(has_down)
                def _():
                    edge_copy(a, False).start()
            return carry

        lax.fori_loop(0, FL, step, 0)

    with jax.named_scope("norm03"):
        normalize((0, 3))
    with jax.named_scope("norm12"):
        normalize((1, 2))
    with jax.named_scope("keys03"):
        keys((0, 3))
    with jax.named_scope("attend03"):
        attend((0, 3), True)
    with jax.named_scope("keys12"):
        keys((1, 2))
    with jax.named_scope("attend12"):
        attend((1, 2), False)

    for copy in loads[6:]:
        copy.wait()

    def first_step(a, carry):
        for r in range(1, 5):
            pads(xp, a, r)

        @pl.when(has_up)
        def _():
            with jax.named_scope("edge_wait_up"):
                edge_copy(a, False).wait_recv()
            pads(xp, a, 0)

        @pl.when(has_down)
        def _():
            with jax.named_scope("edge_wait_down"):
                edge_copy(a, True).wait_recv()
            pads(xp, a, 5)

        weight = cw1[...].reshape(9 * C, C)
        for y in (0, 2):
            result = jnp.dot(taps(xp, a, y, 2), weight, preferred_element_type=F32)
            result = jnp.maximum(result, 0.0).astype(BF)
            yp[a, 1 + y : 3 + y, 16:272, :] = result.reshape(2, 256, C)
        for r in range(1, 5):
            pads(yp, a, r)
        near = cb[a].reshape(256, C)
        for side, row, dy in ((0, 1, 2), (1, 4, 0)):
            lhs = jnp.concatenate([yp[a, row, 16 * dx : 16 * dx + 256, :] for dx in range(3)], axis=1)
            part = jnp.dot(lhs, cw2[dy].reshape(3 * C, C), preferred_element_type=F32)
            part = part + jnp.dot(mats[8 + side], near, preferred_element_type=F32)
            psend[side, a] = part.astype(BF)

        @pl.when(has_up)
        def _():
            part_copy(a, True).start()

        @pl.when(has_down)
        def _():
            part_copy(a, False).start()

        return carry

    with jax.named_scope("first"):
        lax.fori_loop(0, FL, first_step, 0)

    def second_step(a, carry):
        near = cb[a].reshape(256, C)
        inner = jnp.dot(taps(yp, a, 1, 2), cw2[...].reshape(9 * C, C), preferred_element_type=F32)
        outer = []
        for row, first, dys in ((0, 1, (1, 2)), (3, 3, (0, 1))):
            parts = [yp[a, first + k, 16 * dx : 16 * dx + 256, :] for k in range(2) for dx in range(3)]
            weight = cw2[dys[0] : dys[0] + 2].reshape(6 * C, C)
            outer.append(jnp.dot(jnp.concatenate(parts, axis=1), weight, preferred_element_type=F32))
        up = jnp.dot(mats[4:8].reshape(4 * 256, 256), near, preferred_element_type=F32)
        for row, value in ((1, inner[0:256]), (2, inner[256:512]), (0, outer[0]), (3, outer[1])):
            value = value + up[256 * row : 256 * row + 256] + fp[a, row].astype(F32)
            if row in (1, 2):
                fp[a, row] = value.astype(BF)
            else:
                acc[a, row // 3] = value
        return carry

    with jax.named_scope("second"):
        lax.fori_loop(0, FL, second_step, 0)

    def edge_part(a, side):
        near = cb[a].reshape(256, C)
        precv[1 - side, a] = jnp.dot(mats[8 + side], near, preferred_element_type=F32).astype(BF)

    def last_step(a, carry):
        @pl.when(has_up)
        def _():
            with jax.named_scope("part_wait_up"):
                part_copy(a, False).wait_recv()

        @pl.when(jnp.logical_not(has_up))
        def _():
            edge_part(a, 0)

        @pl.when(has_down)
        def _():
            with jax.named_scope("part_wait_down"):
                part_copy(a, True).wait_recv()

        @pl.when(jnp.logical_not(has_down))
        def _():
            edge_part(a, 1)

        for row, side in ((0, 1), (3, 0)):
            value = (acc[a, row // 3] + precv[side, a].astype(F32)).astype(BF)
            ob[a, row] = jnp.dot(mats[0], value, preferred_element_type=F32).astype(BF)
        return carry

    def restore_step(a, carry):
        for row in (1, 2):
            ob[a, row] = jnp.dot(mats[0], fp[a, row], preferred_element_type=F32).astype(BF)
        return carry

    with jax.named_scope("restore"):
        lax.fori_loop(0, FL, restore_step, 0)
    with jax.named_scope("last"):
        lax.fori_loop(0, FL, last_step, 0)

    def drain(a, carry):
        for r in range(RL):
            norm_copy(a, r).wait_send()

        @pl.when(has_up)
        def _():
            edge_copy(a, True).wait_send()
            part_copy(a, True).wait_send()

        @pl.when(has_down)
        def _():
            edge_copy(a, False).wait_send()
            part_copy(a, False).wait_send()

        return carry

    with jax.named_scope("drain"):
        lax.fori_loop(0, FL, drain, 0)


def solution(mesh):
    spaces = mesh.shape["space"]
    constants = tables()
    place = positions()

    def local(fine, coarse, w_query, w_key, w_value, w_out, conv_first, conv_second):
        anywhere = pl.BlockSpec(memory_space=pl.ANY)
        dma = pltpu.SemaphoreType.DMA
        shape = (FL, RL, W, C)
        mats = jnp.asarray(constants)
        moved = pl.pallas_call(
            lambda *refs: kernel(spaces, *refs),
            out_shape=pltpu.VMEM(shape, BF),
            in_specs=[anywhere] * 10,
            out_specs=pl.BlockSpec(memory_space=pltpu.VMEM),
            scratch_shapes=[
                pltpu.VMEM(shape, BF),
                pltpu.VMEM((FL, 2, 128, C), BF),
                pltpu.VMEM((4, C, C), BF),
                pltpu.VMEM((10, 256, 256), BF),
                pltpu.VMEM((8, 1, C), F32),
                pltpu.VMEM((3, 3, C, C), BF),
                pltpu.VMEM((3, 3, C, C), BF),
                pltpu.VMEM((C, C), BF),
                pltpu.VMEM((C, 2 * C), BF),
                pltpu.VMEM((C, C), BF),
                pltpu.VMEM((2 * FL, RL, W, C), BF),
                pltpu.VMEM(shape, BF),
                pltpu.VMEM((2, FL, W, C), BF),
                pltpu.VMEM((2, 2 * FL, W, C), BF),
                pltpu.VMEM((2, 2 * FL, W, C), BF),
                pltpu.VMEM((2, W, C), BF),
                pltpu.VMEM((FL, RL + 2, W + 32, C), BF),
                pltpu.VMEM((FL, RL + 2, W + 32, C), BF),
                pltpu.VMEM((FL, 2, W, C), F32),
                pltpu.VMEM((2, FL, W, C), BF),
                pltpu.VMEM((2, FL, W, C), BF),
                dma((9,)),
                dma((RL,)),
                dma((FL, RL)),
                dma((FL, RL)),
                dma((2, FL)),
                dma((2, FL)),
                dma((2, FL)),
                dma((2, FL)),
            ],
            compiler_params=pltpu.CompilerParams(
                collective_id=0, has_side_effects=True, vmem_limit_bytes=60 * 1024 * 1024),
            name="fused",
        )(fine, coarse, w_query, w_key, w_value, w_out, conv_first, conv_second, mats, jnp.asarray(place))
        def emit(x, o, sem):
            copy = pltpu.make_async_copy(x, o, sem)
            copy.start()
            copy.wait()

        return pl.pallas_call(
            emit,
            out_shape=jax.ShapeDtypeStruct(shape, BF),
            in_specs=[pl.BlockSpec(memory_space=pltpu.VMEM)],
            out_specs=anywhere,
            scratch_shapes=[dma],
            name="emit",
        )(pltpu.with_memory_space_constraint(moved, pltpu.VMEM))

    return jax.shard_map(
        local,
        mesh=mesh,
        in_specs=(P("tm", "space", None, None), P("tm", "space", None, None), P(), P(), P(), P(), P(), P()),
        out_specs=P("tm", "space", None, None),
        check_vma=False,
    )
```

```python
import numpy as np
import jax
import jax.numpy as jnp
from jax import lax
from jax.experimental import pallas as pl
from jax.experimental.pallas import tpu as pltpu
from jax.sharding import PartitionSpec as P

HEADS = 8
C = 256
W = 256
FL = 4
RL = 4
BF = jnp.bfloat16
F32 = jnp.float32
MESH = pl.DeviceIdType.MESH


def tables():
    at = np.arange(256)
    col_of = (at % 16) * 16 + at // 16
    columns = np.zeros((256, 256), np.float32)
    columns[at, col_of] = 1.0
    channel = np.zeros((256, 256), np.float32)
    channel[at, (at % 32) * 8 + at // 32] = 1.0
    same = (at[:, None] // 128 == at[None, :] // 128) & (at[:, None] % 8 == at[None, :] % 8)
    heads = same.astype(np.float32)
    widen = np.zeros((256, 128), np.float32)
    for col in range(256):
        half = col // 2
        other = max(half - 1, 0) if col % 2 == 0 else min(half + 1, 127)
        widen[col, half] += 0.75
        widen[col, other] += 0.25
    widen = widen[col_of]
    none = np.zeros_like(widen)

    def pair(first, second):
        return np.concatenate([first * widen, second * widen], axis=1)

    stack = [columns, channel, channel.T, heads, pair(0.75, 0), pair(0.75, 0.25), pair(0.25, 0.75), pair(0, 0.75), pair(0.25, 0), pair(0, 0.25)]
    return np.stack(stack).astype(jnp.bfloat16)


def positions():
    half = C // 2
    inverse = np.exp(-np.log(10000.0) * 2.0 * np.arange(half) / C)
    angles = np.arange(8)[:, None] * inverse[None, :]
    return np.concatenate([np.sin(angles), np.cos(angles)], axis=1).astype(np.float32)[:, None, :]


def taps(ref, lead, first, rows):
    parts = []
    for dy in range(3):
        for dx in range(3):
            parts.append(ref[lead, first + dy : first + dy + rows, 16 * dx : 16 * dx + 256, :].reshape(rows * 256, C))
    return jnp.concatenate(parts, axis=1)


def pads(ref, lead, row):
    index = lax.broadcasted_iota(jnp.int32, (16, C), 0)
    last = ref[lead, row, 256:272, :].astype(F32)
    before = jnp.where(index == 0, 0.0, pltpu.roll(last, 1, axis=0))
    ref[lead, row, 0:16, :] = before.astype(BF)
    leading = ref[lead, row, 16:32, :].astype(F32)
    after = jnp.where(index == 15, 0.0, pltpu.roll(leading, 15, axis=0))
    ref[lead, row, 272:288, :] = after.astype(BF)


def kernel(
    spaces,
    fine_hbm, coarse_hbm, wq_hbm, wk_hbm, wv_hbm, wo_hbm, c1_hbm, c2_hbm, mats_hbm, pos_hbm,
    ob,
    fin, cb, raw, mats, pos, cw1, cw2,
    wqp, wkv, wop, nbuf, fp, qs, kb, vb, att, xp, yp, acc, psend, precv,
    load_sem, row_sem, nsend, nrecv, xsend, xrecv, tsend, trecv, near_sem, far_sem,
):
    t = lax.axis_index("tm")
    s = lax.axis_index("space")
    has_up = s > 0
    has_down = s < spaces - 1

    def row_load(r):
        return pltpu.make_async_copy(fine_hbm.at[:, r], fin.at[:, r], row_sem.at[r])

    loads = [
        pltpu.make_async_copy(mats_hbm.at[0], mats.at[0], load_sem.at[0]),
        pltpu.make_async_copy(pos_hbm, pos, load_sem.at[1]),
        pltpu.make_async_copy(wq_hbm, raw.at[0], load_sem.at[2]),
        pltpu.make_async_copy(wk_hbm, raw.at[1], load_sem.at[3]),
        pltpu.make_async_copy(wv_hbm, raw.at[2], load_sem.at[4]),
        pltpu.make_async_copy(wo_hbm, raw.at[3], load_sem.at[5]),
        pltpu.make_async_copy(mats_hbm.at[pl.ds(1, 9)], mats.at[pl.ds(1, 9)], load_sem.at[9]),
        pltpu.make_async_copy(coarse_hbm, cb, load_sem.at[6]),
        pltpu.make_async_copy(c1_hbm, cw1, load_sem.at[7]),
        pltpu.make_async_copy(c2_hbm, cw2, load_sem.at[8]),
    ]
    loads[0].start()
    loads[1].start()
    row_load(0).start()
    row_load(3).start()

    barrier = pltpu.get_barrier_semaphore()

    @pl.when(t == 1)
    def _():
        pl.semaphore_signal(barrier, inc=1, device_id=(1 - t, s), device_id_type=MESH)

    for copy in loads[2:7]:
        copy.start()
    row_load(1).start()
    row_load(2).start()
    for copy in loads[7:]:
        copy.start()

    @pl.when(t == 0)
    def _():
        pl.semaphore_wait(barrier, 1)
        pl.semaphore_signal(near_sem, inc=1, device_id=(1 - t, s), device_id_type=MESH)

    @pl.when(t == 1)
    def _():
        pl.semaphore_wait(near_sem, 1)

    @pl.when(jnp.logical_and(t == 1, has_up))
    def _():
        pl.semaphore_signal(barrier, inc=1, device_id=(t, s - 1), device_id_type=MESH)

    @pl.when(jnp.logical_and(t == 1, has_down))
    def _():
        pl.semaphore_signal(barrier, inc=1, device_id=(t, s + 1), device_id_type=MESH)

    def meet_neighbours():
        @pl.when(t == 1)
        def _():
            pl.semaphore_wait(barrier, has_up.astype(jnp.int32) + has_down.astype(jnp.int32))
            pl.semaphore_signal(far_sem, inc=1, device_id=(1 - t, s), device_id_type=MESH)

        @pl.when(t == 0)
        def _():
            pl.semaphore_wait(far_sem, 1)

    zero_row = jnp.zeros((FL, 288, C), BF)

    @pl.when(jnp.logical_not(has_up))
    def _():
        xp[:, 0] = zero_row

    @pl.when(jnp.logical_not(has_down))
    def _():
        xp[:, 5] = zero_row

    def norm_copy(k):
        r = (0, 3, 0, 3, 1, 2)[k]
        px = pl.ds((0, 0, 128, 128, 0, 0)[k], 128 if k < 4 else 256)
        return pltpu.make_async_remote_copy(
            src_ref=nbuf.at[pl.ds(0, FL), r, px], dst_ref=nbuf.at[pl.ds(FL, FL), r, px],
            send_sem=nsend.at[k], recv_sem=nrecv.at[k],
            device_id=(1 - t, s), device_id_type=MESH)

    def normalize(units, start, count):
        px = slice(start, start + count)
        placed = [jnp.dot(mats[0, px], fin[f, r], preferred_element_type=F32) for f, r in units]
        for (f, r), moved in zip(units, placed):
            fp[f, r, px] = moved.astype(BF)
            hidden = moved + pos[t * FL + f]
            center = hidden - jnp.mean(hidden, axis=-1, keepdims=True)
            spread = jnp.mean(center * center, axis=-1, keepdims=True)
            nbuf[f, r, px] = (center * lax.rsqrt(spread + 1e-05)).astype(BF)

    def edge_copy(a, up, h):
        row, slot, to = (1, 5, s - 1) if up else (4, 0, s + 1)
        side = 0 if up else 1
        px = pl.ds(16 + 128 * h, 128)
        return pltpu.make_async_remote_copy(
            src_ref=xp.at[a, row, px], dst_ref=xp.at[a, slot, px],
            send_sem=xsend.at[side, a, h], recv_sem=xrecv.at[side, a, h],
            device_id=(t, to), device_id_type=MESH)

    def part_copy(a, up):
        side = 0 if up else 1
        to = s - 1 if up else s + 1
        return pltpu.make_async_remote_copy(
            src_ref=psend.at[side, a], dst_ref=precv.at[side, a],
            send_sem=tsend.at[side, a], recv_sem=trecv.at[side, a],
            device_id=(t, to), device_id_type=MESH)

    factor = float(np.log2(np.e) / np.sqrt(32.0))

    def project(rows, frames, own, start, count):
        px = slice(start, start + count)
        units = [(b, r) for b in frames for r in rows]
        stacked = jnp.concatenate([nbuf[b, r, px] for b, r in units], axis=0)
        both = jnp.dot(stacked, wkv[...], preferred_element_type=F32)
        if own:
            query = jnp.dot(stacked, wqp[...], preferred_element_type=F32)
        for i, (b, r) in enumerate(units):
            at = slice(count * i, count * i + count)
            kb[r, b, px] = both[at, 0:256].astype(BF)
            vb[r, b, px] = both[at, 256:512].astype(BF)
            if own:
                qs[r, b, px] = (query[at] * factor).astype(BF)

    def weigh(a, r, start, into):
        px = slice(start, start + 64)
        out = slice(into, into + 64)
        q = qs[r, a, px]
        lhs = []
        for pair in range(4):
            halves = []
            for b in (2 * pair, 2 * pair + 1):
                product = q * kb[r, b, px]
                halves.append(product[:, 0:128] + product[:, 128:256])
            lhs.append(jnp.concatenate(halves, axis=1))
        both = jnp.dot(jnp.concatenate(lhs, axis=0), mats[3], preferred_element_type=F32)
        scores = []
        for b in range(8):
            at = 64 * (b // 2)
            scores.append(both[at : at + 64, 128 * (b % 2) : 128 * (b % 2) + 128])
        largest = scores[0]
        for entry in scores[1:]:
            largest = jnp.maximum(largest, entry)
        powers = [jnp.exp2(entry - largest) for entry in scores]
        total = powers[0]
        for entry in powers[1:]:
            total = total + entry
        inverse = 1.0 / total
        low, high = [], []
        for b in range(8):
            weight = powers[b].astype(BF)
            value = vb[r, b, px]
            low.append(weight * value[:, 0:128])
            high.append(weight * value[:, 128:256])
        while len(low) > 1:
            low = [low[j] + low[j + 1] for j in range(0, len(low), 2)]
            high = [high[j] + high[j + 1] for j in range(0, len(high), 2)]
        att[out, 0:128] = (low[0].astype(F32) * inverse).astype(BF)
        att[out, 128:256] = (high[0].astype(F32) * inverse).astype(BF)

    def attend(units, count, beside=()):
        beside = list(beside)
        into = 0
        for a, r, start in units:
            for px in range(start, start + count, 64):
                weigh(a, r, px, into)
                into += 64
                if into % 128 == 0 and beside:
                    beside.pop(0)()
        for run in beside:
            run()
        branch = jnp.dot(att[...], wop[...], preferred_element_type=F32)
        for i, (a, r, start) in enumerate(units):
            px = slice(start, start + count)
            moved = (fp[a, r, px].astype(F32) + branch[count * i : count * i + count]).astype(BF)
            fp[a, r, px] = moved
            xp[a, r + 1, 16 + start : 16 + start + count, :] = jnp.maximum(moved, jnp.zeros_like(moved))

    def send_edges(a, h):
        @pl.when(has_up)
        def _():
            edge_copy(a, True, h).start()

        @pl.when(has_down)
        def _():
            edge_copy(a, False, h).start()

    def wait_norms(ks):
        with jax.named_scope("norm_wait"):
            for k in ks:
                norm_copy(k).wait_recv()

    def first_wait(a):
        @pl.when(has_up)
        def _():
            with jax.named_scope("edge_wait_up"):
                for h in range(2):
                    edge_copy(a, False, h).wait_recv()

        @pl.when(has_down)
        def _():
            with jax.named_scope("edge_wait_down"):
                for h in range(2):
                    edge_copy(a, True, h).wait_recv()

    def first_rows(a):
        weight = cw1[...].reshape(9 * C, C)

        def run(y):
            result = jnp.dot(taps(xp, a, y, 1), weight, preferred_element_type=F32)
            yp[a, 1 + y, 16:272, :] = jnp.maximum(result, 0.0).astype(BF)

        return [lambda y=y: run(y) for y in (0, 3, 1, 2)]

    def first_end(a):
        for r in range(1, 5):
            pads(yp, a, r)
        near = cb[a].reshape(256, C)
        parts = []
        for side, row, dy in ((0, 1, 2), (1, 4, 0)):
            lhs = jnp.concatenate([yp[a, row, 16 * dx : 16 * dx + 256, :] for dx in range(3)], axis=1)
            parts.append(jnp.dot(lhs, cw2[dy].reshape(3 * C, C), preferred_element_type=F32))
        for side in (0, 1):
            parts[side] = parts[side] + jnp.dot(mats[8 + side], near, preferred_element_type=F32)
        for side in (0, 1):
            psend[side, a] = parts[side].astype(BF)

    def send_parts(a):
        @pl.when(has_up)
        def _():
            part_copy(a, True).start()

        @pl.when(has_down)
        def _():
            part_copy(a, False).start()

    with jax.named_scope("load_wait"):
        loads[0].wait()
        loads[1].wait()
        row_load(0).wait()
        row_load(3).wait()
    edge_units = [(f, r) for f in range(FL) for r in (0, 3)]
    with jax.named_scope("norm03"):
        normalize(edge_units, 0, 128)
    norm_copy(0).start()
    norm_copy(1).start()
    with jax.named_scope("norm03b"):
        normalize(edge_units, 128, 128)
    norm_copy(2).start()
    norm_copy(3).start()
    with jax.named_scope("weights"):
        for copy in loads[2:7]:
            copy.wait()
        wqp[...] = jnp.dot(raw[0], mats[1], preferred_element_type=F32).astype(BF)
        wkv[:, 0:256] = jnp.dot(raw[1], mats[1], preferred_element_type=F32).astype(BF)
        wkv[:, 256:512] = jnp.dot(raw[2], mats[1], preferred_element_type=F32).astype(BF)
        wop[...] = jnp.dot(mats[2], raw[3], preferred_element_type=F32).astype(BF)
    with jax.named_scope("keys03"):
        project((0, 3), range(0, 4), True, 0, 128)
    wait_norms((0, 1))
    with jax.named_scope("keys03b"):
        project((0, 3), range(4, 8), False, 0, 128)

    def edge_pair(k, h, beside, meet=False):
        frames = (2 * k, 2 * k + 1)
        attend([(a, r, 128 * h) for a in frames for r in (0, 3)], 128, beside)
        if meet:
            with jax.named_scope("meet"):
                meet_neighbours()
        for a in frames:
            send_edges(a, h)

    with jax.named_scope("attend03"):
        edge_pair(0, 0, [lambda k=k: project((0, 3), (2 * k, 2 * k + 1), True, 128, 128) for k in range(2)], True)
    row_load(1).wait()
    row_load(2).wait()

    def inner_norm(pair, carry):
        normalize([(2 * pair + k, r) for k in range(2) for r in (1, 2)], 0, 256)
        return carry

    with jax.named_scope("norm12"):
        lax.fori_loop(0, 2, inner_norm, 0)
    norm_copy(4).start()
    norm_copy(5).start()
    wait_norms((2, 3))
    with jax.named_scope("attend03b"):
        project((0, 3), range(4, 8), False, 128, 128)
        edge_pair(0, 1, [])
    with jax.named_scope("attend03c"):
        edge_pair(1, 0, [lambda b=b: project((1, 2), (b,), True, 0, 256) for b in range(0, 4)])
    wait_norms((4, 5))
    with jax.named_scope("attend03d"):
        edge_pair(1, 1, [lambda b=b: project((1, 2), (b,), False, 0, 256) for b in range(4, 8)])
    with jax.named_scope("attend12"):
        attend([(0, 1, 0), (0, 2, 0)], 256)
    for copy in loads[7:]:
        copy.wait()

    def mixed_step(a, carry):
        first_wait(a)
        for r in range(6):
            pads(xp, a, r)
        attend([(a + 1, 1, 0), (a + 1, 2, 0)], 256, first_rows(a))
        first_end(a)
        send_parts(a)
        return carry

    with jax.named_scope("mixed"):
        lax.fori_loop(0, FL - 1, mixed_step, 0)
    with jax.named_scope("first"):
        first_wait(FL - 1)
        for r in range(6):
            pads(xp, FL - 1, r)
        for run in first_rows(FL - 1):
            run()
        first_end(FL - 1)
        send_parts(FL - 1)

    def second_step(a, carry):
        near = cb[a].reshape(256, C)
        inner = jnp.dot(taps(yp, a, 1, 2), cw2[...].reshape(9 * C, C), preferred_element_type=F32)
        outer = []
        for row, first, dys in ((0, 1, (1, 2)), (3, 3, (0, 1))):
            parts = [yp[a, first + k, 16 * dx : 16 * dx + 256, :] for k in range(2) for dx in range(3)]
            weight = cw2[dys[0] : dys[0] + 2].reshape(6 * C, C)
            outer.append(jnp.dot(jnp.concatenate(parts, axis=1), weight, preferred_element_type=F32))
        up = jnp.dot(mats[4:8].reshape(4 * 256, 256), near, preferred_element_type=F32)
        for row, value in ((1, inner[0:256]), (2, inner[256:512]), (0, outer[0]), (3, outer[1])):
            value = value + up[256 * row : 256 * row + 256] + fp[a, row].astype(F32)
            if row in (1, 2):
                fp[a, row] = value.astype(BF)
            else:
                acc[a, row // 3] = value
        return carry

    with jax.named_scope("second"):
        lax.fori_loop(0, FL, second_step, 0)

    def edge_part(a, side):
        near = cb[a].reshape(256, C)
        precv[1 - side, a] = jnp.dot(mats[8 + side], near, preferred_element_type=F32).astype(BF)

    def last_step(a, carry):
        @pl.when(has_up)
        def _():
            with jax.named_scope("part_wait_up"):
                part_copy(a, False).wait_recv()

        @pl.when(jnp.logical_not(has_up))
        def _():
            edge_part(a, 0)

        @pl.when(has_down)
        def _():
            with jax.named_scope("part_wait_down"):
                part_copy(a, True).wait_recv()

        @pl.when(jnp.logical_not(has_down))
        def _():
            edge_part(a, 1)

        for row, side in ((0, 1), (3, 0)):
            value = (acc[a, row // 3] + precv[side, a].astype(F32)).astype(BF)
            ob[a, row] = jnp.dot(mats[0], value, preferred_element_type=F32).astype(BF)
        return carry

    def restore_step(a, carry):
        for row in (1, 2):
            ob[a, row] = jnp.dot(mats[0], fp[a, row], preferred_element_type=F32).astype(BF)
        return carry

    with jax.named_scope("restore"):
        lax.fori_loop(0, FL, restore_step, 0)
    with jax.named_scope("last"):
        lax.fori_loop(0, FL, last_step, 0)

    def drain(a, carry):

        @pl.when(has_up)
        def _():
            for h in range(2):
                edge_copy(a, True, h).wait_send()
            part_copy(a, True).wait_send()

        @pl.when(has_down)
        def _():
            for h in range(2):
                edge_copy(a, False, h).wait_send()
            part_copy(a, False).wait_send()

        return carry

    for k in range(6):
        norm_copy(k).wait_send()
    with jax.named_scope("drain"):
        lax.fori_loop(0, FL, drain, 0)


def solution(mesh):
    spaces = mesh.shape["space"]
    constants = tables()
    place = positions()

    def local(fine, coarse, w_query, w_key, w_value, w_out, conv_first, conv_second):
        anywhere = pl.BlockSpec(memory_space=pl.ANY)
        dma = pltpu.SemaphoreType.DMA
        shape = (FL, RL, W, C)
        mats = jnp.asarray(constants)
        moved = pl.pallas_call(
            lambda *refs: kernel(spaces, *refs),
            out_shape=pltpu.VMEM(shape, BF),
            in_specs=[anywhere] * 10,
            out_specs=pl.BlockSpec(memory_space=pltpu.VMEM),
            scratch_shapes=[
                pltpu.VMEM(shape, BF),
                pltpu.VMEM((FL, 2, 128, C), BF),
                pltpu.VMEM((4, C, C), BF),
                pltpu.VMEM((10, 256, 256), BF),
                pltpu.VMEM((8, 1, C), F32),
                pltpu.VMEM((3, 3, C, C), BF),
                pltpu.VMEM((3, 3, C, C), BF),
                pltpu.VMEM((C, C), BF),
                pltpu.VMEM((C, 2 * C), BF),
                pltpu.VMEM((C, C), BF),
                pltpu.VMEM((2 * FL, RL, W, C), BF),
                pltpu.VMEM(shape, BF),
                pltpu.VMEM((RL, FL, W, C), BF),
                pltpu.VMEM((RL, 2 * FL, W, C), BF),
                pltpu.VMEM((RL, 2 * FL, W, C), BF),
                pltpu.VMEM((2 * W, C), BF),
                pltpu.VMEM((FL, RL + 2, W + 32, C), BF),
                pltpu.VMEM((FL, RL + 2, W + 32, C), BF),
                pltpu.VMEM((FL, 2, W, C), F32),
                pltpu.VMEM((2, FL, W, C), BF),
                pltpu.VMEM((2, FL, W, C), BF),
                dma((10,)),
                dma((RL,)),
                dma((6,)),
                dma((6,)),
                dma((2, FL, 2)),
                dma((2, FL, 2)),
                dma((2, FL)),
                dma((2, FL)),
                pltpu.SemaphoreType.REGULAR,
                pltpu.SemaphoreType.REGULAR,
            ],
            compiler_params=pltpu.CompilerParams(
                collective_id=0, has_side_effects=True, vmem_limit_bytes=60 * 1024 * 1024),
            name="fused",
        )(fine, coarse, w_query, w_key, w_value, w_out, conv_first, conv_second, mats, jnp.asarray(place))
        def emit(x, o, sem):
            copy = pltpu.make_async_copy(x, o, sem)
            copy.start()
            copy.wait()

        return pl.pallas_call(
            emit,
            out_shape=jax.ShapeDtypeStruct(shape, BF),
            in_specs=[pl.BlockSpec(memory_space=pltpu.VMEM)],
            out_specs=anywhere,
            scratch_shapes=[dma],
            name="emit",
        )(pltpu.with_memory_space_constraint(moved, pltpu.VMEM))

    return jax.shard_map(
        local,
        mesh=mesh,
        in_specs=(P("tm", "space", None, None), P("tm", "space", None, None), P(), P(), P(), P(), P(), P()),
        out_specs=P("tm", "space", None, None),
        check_vma=False,
    )
```

```python
import numpy as np
import jax
import jax.numpy as jnp
from jax import lax
from jax.experimental import pallas as pl
from jax.experimental.pallas import tpu as pltpu
from jax.sharding import PartitionSpec as P

HEADS = 8
C = 256
W = 256
FL = 4
RL = 4
BF = jnp.bfloat16
F32 = jnp.float32
MESH = pl.DeviceIdType.MESH


def tables():
    at = np.arange(256)
    col_of = (at % 16) * 16 + at // 16
    columns = np.zeros((256, 256), np.float32)
    columns[at, col_of] = 1.0
    channel = np.zeros((256, 256), np.float32)
    channel[at, (at % 32) * 8 + at // 32] = 1.0
    same = (at[:, None] // 128 == at[None, :] // 128) & (at[:, None] % 8 == at[None, :] % 8)
    heads = same.astype(np.float32)
    widen = np.zeros((256, 128), np.float32)
    for col in range(256):
        half = col // 2
        other = max(half - 1, 0) if col % 2 == 0 else min(half + 1, 127)
        widen[col, half] += 0.75
        widen[col, other] += 0.25
    widen = widen[col_of]
    none = np.zeros_like(widen)

    def pair(first, second):
        return np.concatenate([first * widen, second * widen], axis=1)

    stack = [columns, channel, channel.T, heads, pair(0.75, 0), pair(0.75, 0.25), pair(0.25, 0.75), pair(0, 0.75), pair(0.25, 0), pair(0, 0.25)]
    return np.stack(stack).astype(jnp.bfloat16)


def positions():
    half = C // 2
    inverse = np.exp(-np.log(10000.0) * 2.0 * np.arange(half) / C)
    angles = np.arange(8)[:, None] * inverse[None, :]
    return np.concatenate([np.sin(angles), np.cos(angles)], axis=1).astype(np.float32)[:, None, :]


def taps(ref, lead, first, rows):
    parts = []
    for dy in range(3):
        for dx in range(3):
            parts.append(ref[lead, first + dy : first + dy + rows, 16 * dx : 16 * dx + 256, :].reshape(rows * 256, C))
    return jnp.concatenate(parts, axis=1)


def pads(ref, lead, row):
    index = lax.broadcasted_iota(jnp.int32, (16, C), 0)
    last = ref[lead, row, 256:272, :].astype(F32)
    before = jnp.where(index == 0, 0.0, pltpu.roll(last, 1, axis=0))
    ref[lead, row, 0:16, :] = before.astype(BF)
    leading = ref[lead, row, 16:32, :].astype(F32)
    after = jnp.where(index == 15, 0.0, pltpu.roll(leading, 15, axis=0))
    ref[lead, row, 272:288, :] = after.astype(BF)


def kernel(
    spaces,
    fine_hbm, coarse_hbm, wq_hbm, wk_hbm, wv_hbm, wo_hbm, c1_hbm, c2_hbm, mats_hbm, pos_hbm,
    ob,
    fin, cb, raw, mats, pos, cw1, cw2,
    wqp, wkv, wop, nbuf, fp, qs, kb, vb, att, xp, yp, acc, psend, precv,
    load_sem, row_sem, nsend, nrecv, xsend, xrecv, tsend, trecv, near_sem, far_sem,
):
    t = lax.axis_index("tm")
    s = lax.axis_index("space")
    has_up = s > 0
    has_down = s < spaces - 1

    def row_load(r):
        return pltpu.make_async_copy(fine_hbm.at[:, r], fin.at[:, r], row_sem.at[r])

    loads = [
        pltpu.make_async_copy(mats_hbm.at[pl.ds(0, 3)], mats.at[pl.ds(0, 3)], load_sem.at[0]),
        pltpu.make_async_copy(mats_hbm.at[pl.ds(0, 4)], raw, load_sem.at[1]),
        pltpu.make_async_copy(pos_hbm, pos, load_sem.at[2]),
        pltpu.make_async_copy(mats_hbm.at[pl.ds(3, 7)], mats.at[pl.ds(3, 7)], load_sem.at[3]),
        pltpu.make_async_copy(coarse_hbm, cb, load_sem.at[4]),
        pltpu.make_async_copy(c1_hbm, cw1, load_sem.at[5]),
        pltpu.make_async_copy(c2_hbm, cw2, load_sem.at[6]),
    ]
    loads[0].start()
    for k, weight in enumerate((wq_hbm, wk_hbm, wv_hbm, wo_hbm)):
        pltpu.make_async_copy(weight, raw.at[k], load_sem.at[1]).start()
    loads[2].start()
    row_load(0).start()
    row_load(3).start()

    barrier = pltpu.get_barrier_semaphore()

    @pl.when(t == 1)
    def _():
        pl.semaphore_signal(barrier, inc=1, device_id=(1 - t, s), device_id_type=MESH)

    loads[3].start()
    row_load(1).start()
    row_load(2).start()
    for copy in loads[4:]:
        copy.start()

    @pl.when(t == 0)
    def _():
        pl.semaphore_wait(barrier, 1)
        pl.semaphore_signal(near_sem, inc=1, device_id=(1 - t, s), device_id_type=MESH)

    @pl.when(t == 1)
    def _():
        pl.semaphore_wait(near_sem, 1)

    @pl.when(jnp.logical_and(t == 1, has_up))
    def _():
        pl.semaphore_signal(barrier, inc=1, device_id=(t, s - 1), device_id_type=MESH)

    @pl.when(jnp.logical_and(t == 1, has_down))
    def _():
        pl.semaphore_signal(barrier, inc=1, device_id=(t, s + 1), device_id_type=MESH)

    zero_row = jnp.zeros((FL, 288, C), BF)

    @pl.when(jnp.logical_not(has_up))
    def _():
        xp[:, 0] = zero_row

    @pl.when(jnp.logical_not(has_down))
    def _():
        xp[:, 5] = zero_row

    def norm_copy(k):
        r = (0, 3, 0, 3, 1, 2)[k]
        px = pl.ds((0, 0, 128, 128, 0, 0)[k], 128 if k < 4 else 256)
        return pltpu.make_async_remote_copy(
            src_ref=nbuf.at[pl.ds(0, FL), r, px], dst_ref=nbuf.at[pl.ds(FL, FL), r, px],
            send_sem=nsend, recv_sem=nrecv.at[k],
            device_id=(1 - t, s), device_id_type=MESH)

    def normalize(units, start, count):
        px = slice(start, start + count)
        placed = [jnp.dot(mats[0, px], fin[f, r], preferred_element_type=F32) for f, r in units]
        for (f, r), moved in zip(units, placed):
            fp[f, r, px] = moved.astype(BF)
            hidden = moved + pos[t * FL + f]
            center = hidden - jnp.mean(hidden, axis=-1, keepdims=True)
            spread = jnp.mean(center * center, axis=-1, keepdims=True)
            nbuf[f, r, px] = (center * lax.rsqrt(spread + 1e-05)).astype(BF)

    def edge_copy(a, up, h):
        row, slot, to = (1, 5, s - 1) if up else (4, 0, s + 1)
        side = 0 if up else 1
        px = pl.ds(16 + 128 * h, 128)
        return pltpu.make_async_remote_copy(
            src_ref=xp.at[a, row, px], dst_ref=xp.at[a, slot, px],
            send_sem=xsend.at[side], recv_sem=xrecv.at[side, a, h],
            device_id=(t, to), device_id_type=MESH)

    def part_copy(a, up):
        side = 0 if up else 1
        to = s - 1 if up else s + 1
        return pltpu.make_async_remote_copy(
            src_ref=psend.at[side, a], dst_ref=precv.at[side, a],
            send_sem=tsend.at[side], recv_sem=trecv.at[side, a],
            device_id=(t, to), device_id_type=MESH)

    factor = float(np.log2(np.e) / np.sqrt(32.0))

    def project(rows, frames, own, start, count):
        px = slice(start, start + count)
        units = [(b, r) for b in frames for r in rows]
        stacked = jnp.concatenate([nbuf[b, r, px] for b, r in units], axis=0)
        both = jnp.dot(stacked, wkv[...], preferred_element_type=F32)
        if own:
            query = jnp.dot(stacked, wqp[...], preferred_element_type=F32)
        for i, (b, r) in enumerate(units):
            at = slice(count * i, count * i + count)
            kb[r, b, px] = both[at, 0:256].astype(BF)
            vb[r, b, px] = both[at, 256:512].astype(BF)
            if own:
                qs[r, b, px] = (query[at] * factor).astype(BF)

    def weigh(a, r, start, into):
        px = slice(start, start + 64)
        out = slice(into, into + 64)
        q = qs[r, a, px]
        lhs = []
        for pair in range(4):
            halves = []
            for b in (2 * pair, 2 * pair + 1):
                product = q * kb[r, b, px]
                halves.append(product[:, 0:128] + product[:, 128:256])
            lhs.append(jnp.concatenate(halves, axis=1))
        both = jnp.dot(jnp.concatenate(lhs, axis=0), mats[3], preferred_element_type=F32)
        scores = []
        for b in range(8):
            at = 64 * (b // 2)
            scores.append(both[at : at + 64, 128 * (b % 2) : 128 * (b % 2) + 128])
        largest = scores[0]
        for entry in scores[1:]:
            largest = jnp.maximum(largest, entry)
        powers = [jnp.exp2(entry - largest) for entry in scores]
        total = powers[0]
        for entry in powers[1:]:
            total = total + entry
        inverse = 1.0 / total
        low, high = [], []
        for b in range(8):
            weight = powers[b].astype(BF)
            value = vb[r, b, px]
            low.append(weight * value[:, 0:128])
            high.append(weight * value[:, 128:256])
        while len(low) > 1:
            low = [low[j] + low[j + 1] for j in range(0, len(low), 2)]
            high = [high[j] + high[j + 1] for j in range(0, len(high), 2)]
        att[out, 0:128] = (low[0].astype(F32) * inverse).astype(BF)
        att[out, 128:256] = (high[0].astype(F32) * inverse).astype(BF)

    def attend(units, count, beside=()):
        beside = list(beside)
        into = 0
        for a, r, start in units:
            for px in range(start, start + count, 64):
                weigh(a, r, px, into)
                into += 64
                if into % 128 == 0 and beside:
                    beside.pop(0)()
        for run in beside:
            run()
        branch = jnp.dot(att[0:into], wop[...], preferred_element_type=F32)
        for i, (a, r, start) in enumerate(units):
            px = slice(start, start + count)
            moved = (fp[a, r, px].astype(F32) + branch[count * i : count * i + count]).astype(BF)
            fp[a, r, px] = moved
            xp[a, r + 1, 16 + start : 16 + start + count, :] = jnp.maximum(moved, jnp.zeros_like(moved))

    def send_up(a, h):
        @pl.when(has_up)
        def _():
            edge_copy(a, True, h).start()

    def send_down(a, h):
        @pl.when(has_down)
        def _():
            edge_copy(a, False, h).start()

    def send_edges(a, h):
        send_down(a, h)
        send_up(a, h)

    def wait_norms(ks):
        with jax.named_scope("norm_wait"):
            for k in ks:
                norm_copy(k).wait_recv()

    def first_wait(a):
        @pl.when(has_up)
        def _():
            with jax.named_scope("edge_wait_up"):
                for h in range(2):
                    edge_copy(a, False, h).wait_recv()

        @pl.when(has_down)
        def _():
            with jax.named_scope("edge_wait_down"):
                for h in range(2):
                    edge_copy(a, True, h).wait_recv()

    def first_rows(a, rows):
        weight = cw1[...].reshape(9 * C, C)

        def run(y):
            result = jnp.dot(taps(xp, a, y, 1), weight, preferred_element_type=F32)
            yp[a, 1 + y, 16:272, :] = jnp.maximum(result, 0.0).astype(BF)

        return [lambda y=y: run(y) for y in rows]

    def first_end(a):
        for r in range(1, 5):
            pads(yp, a, r)
        near = cb[a].reshape(256, C)
        parts = []
        for side, row, dy in ((0, 1, 2), (1, 4, 0)):
            lhs = jnp.concatenate([yp[a, row, 16 * dx : 16 * dx + 256, :] for dx in range(3)], axis=1)
            parts.append(jnp.dot(lhs, cw2[dy].reshape(3 * C, C), preferred_element_type=F32))
        for side in (0, 1):
            parts[side] = parts[side] + jnp.dot(mats[8 + side], near, preferred_element_type=F32)
        for side in (0, 1):
            psend[side, a] = parts[side].astype(BF)

    def send_parts(a):
        @pl.when(has_up)
        def _():
            part_copy(a, True).start()

        @pl.when(has_down)
        def _():
            part_copy(a, False).start()

    with jax.named_scope("weights"):
        for copy in loads[:2]:
            copy.wait()
        wqp[...] = jnp.dot(raw[0], mats[1], preferred_element_type=F32).astype(BF)
        wkv[:, 0:256] = jnp.dot(raw[1], mats[1], preferred_element_type=F32).astype(BF)
        wkv[:, 256:512] = jnp.dot(raw[2], mats[1], preferred_element_type=F32).astype(BF)
        wop[...] = jnp.dot(mats[2], raw[3], preferred_element_type=F32).astype(BF)
    with jax.named_scope("load_wait"):
        loads[2].wait()
        row_load(0).wait()
        row_load(3).wait()
    edge_units = [(f, r) for f in range(FL) for r in (0, 3)]
    with jax.named_scope("norm03"):
        normalize(edge_units, 0, 128)
    norm_copy(0).start()
    norm_copy(1).start()
    with jax.named_scope("norm03b"):
        normalize(edge_units, 128, 128)
    norm_copy(2).start()
    norm_copy(3).start()
    with jax.named_scope("keys03"):
        project((0, 3), range(0, 4), True, 0, 128)
    wait_norms((0, 1))
    with jax.named_scope("keys03b"):
        project((0, 3), range(4, 8), False, 0, 128)

    def edge_pair(k, h, beside):
        frames = (2 * k, 2 * k + 1)
        attend([(a, r, 128 * h) for a in frames for r in (0, 3)], 128, beside)
        for a in frames:
            send_edges(a, h)

    loads[3].wait()

    @pl.when(t == 1)
    def _():
        pl.semaphore_wait(barrier, has_up.astype(jnp.int32) + has_down.astype(jnp.int32))
        pl.semaphore_signal(far_sem, inc=1, device_id=(1 - t, s), device_id_type=MESH)

    with jax.named_scope("attend03"):
        attend([(0, 3, 0)], 128)
        with jax.named_scope("meet"):
            @pl.when(t == 0)
            def _():
                pl.semaphore_wait(far_sem, 1)

        send_down(0, 0)
        attend([(0, 0, 0)], 128)
        send_up(0, 0)
        attend([(1, 0, 0), (1, 3, 0)], 128, [lambda k=k: project((0, 3), (2 * k, 2 * k + 1), True, 128, 128) for k in range(2)])
        send_edges(1, 0)
    def inner_norm(pair, carry):
        normalize([(2 * pair + k, r) for k in range(2) for r in (1, 2)], 0, 256)
        return carry

    wait_norms((2, 3))
    with jax.named_scope("attend03b"):
        project((0, 3), range(4, 8), False, 128, 128)
        edge_pair(0, 1, [])
    with jax.named_scope("norm12"):
        row_load(1).wait()
        row_load(2).wait()
        lax.fori_loop(0, 2, inner_norm, 0)
    norm_copy(4).start()
    norm_copy(5).start()
    with jax.named_scope("attend03c"):
        edge_pair(1, 0, [lambda b=b: project((1, 2), (b,), True, 0, 256) for b in range(0, 4)])
    with jax.named_scope("attend03d"):
        edge_pair(1, 1, [])
    wait_norms((4, 5))
    with jax.named_scope("keys12b"):
        for b in range(4, 8, 2):
            project((1, 2), (b, b + 1), False, 0, 256)
    with jax.named_scope("attend12"):
        attend([(0, 1, 0), (0, 2, 0)], 256)
    for copy in loads[4:]:
        copy.wait()

    def mixed_step(a, carry):
        for r in range(1, 5):
            pads(xp, a, r)
        attend([(a + 1, 1, 0), (a + 1, 2, 0)], 256, first_rows(a, (1, 2)))
        first_wait(a)
        outer(a)
        send_parts(a)
        return carry

    def outer(a):
        for r in (0, 5):
            pads(xp, a, r)
        for run in first_rows(a, (0, 3)):
            run()
        first_end(a)

    with jax.named_scope("mixed"):
        lax.fori_loop(0, FL - 1, mixed_step, 0)
    with jax.named_scope("first"):
        for r in range(1, 5):
            pads(xp, FL - 1, r)
        first_wait(FL - 1)
        outer(FL - 1)
        send_parts(FL - 1)
        for run in first_rows(FL - 1, (1, 2)):
            run()
        for r in (2, 3):
            pads(yp, FL - 1, r)

    def second_step(a, carry):
        near = cb[a].reshape(256, C)
        inner = jnp.dot(taps(yp, a, 1, 2), cw2[...].reshape(9 * C, C), preferred_element_type=F32)
        outer = []
        for row, first, dys in ((0, 1, (1, 2)), (3, 3, (0, 1))):
            parts = [yp[a, first + k, 16 * dx : 16 * dx + 256, :] for k in range(2) for dx in range(3)]
            weight = cw2[dys[0] : dys[0] + 2].reshape(6 * C, C)
            outer.append(jnp.dot(jnp.concatenate(parts, axis=1), weight, preferred_element_type=F32))
        up = jnp.dot(mats[4:8].reshape(4 * 256, 256), near, preferred_element_type=F32)
        for row, value in ((1, inner[0:256]), (2, inner[256:512]), (0, outer[0]), (3, outer[1])):
            value = value + up[256 * row : 256 * row + 256] + fp[a, row].astype(F32)
            if row in (1, 2):
                fp[a, row] = value.astype(BF)
            else:
                acc[a, row // 3] = value
        return carry

    with jax.named_scope("second"):
        lax.fori_loop(0, FL, second_step, 0)

    def edge_part(a, side):
        near = cb[a].reshape(256, C)
        precv[1 - side, a] = jnp.dot(mats[8 + side], near, preferred_element_type=F32).astype(BF)

    def last_step(a, carry):
        @pl.when(has_up)
        def _():
            with jax.named_scope("part_wait_up"):
                part_copy(a, False).wait_recv()

        @pl.when(jnp.logical_not(has_up))
        def _():
            edge_part(a, 0)

        @pl.when(has_down)
        def _():
            with jax.named_scope("part_wait_down"):
                part_copy(a, True).wait_recv()

        @pl.when(jnp.logical_not(has_down))
        def _():
            edge_part(a, 1)

        for row, side in ((0, 1), (3, 0)):
            value = (acc[a, row // 3] + precv[side, a].astype(F32)).astype(BF)
            ob[a, row] = jnp.dot(mats[0], value, preferred_element_type=F32).astype(BF)
        return carry

    def restore_step(a, carry):
        for row in (1, 2):
            ob[a, row] = jnp.dot(mats[0], fp[a, row], preferred_element_type=F32).astype(BF)
        return carry

    with jax.named_scope("restore"):
        lax.fori_loop(0, FL, restore_step, 0)
    with jax.named_scope("last"):
        lax.fori_loop(0, FL, last_step, 0)

    with jax.named_scope("drain"):
        pltpu.make_async_remote_copy(
            src_ref=nbuf.at[pl.ds(0, FL)], dst_ref=nbuf.at[pl.ds(FL, FL)], send_sem=nsend, recv_sem=nrecv.at[0],
            device_id=(1 - t, s), device_id_type=MESH).wait_send()
        for side, flag, row, slot, to in ((0, has_up, 1, 5, s - 1), (1, has_down, 4, 0, s + 1)):
            @pl.when(flag)
            def _(side=side, row=row, slot=slot, to=to):
                pltpu.make_async_remote_copy(
                    src_ref=xp.at[:, row, pl.ds(16, 256)], dst_ref=xp.at[:, slot, pl.ds(16, 256)],
                    send_sem=xsend.at[side], recv_sem=xrecv.at[side, 0, 0],
                    device_id=(t, to), device_id_type=MESH).wait_send()
                pltpu.make_async_remote_copy(
                    src_ref=psend.at[side], dst_ref=precv.at[side],
                    send_sem=tsend.at[side], recv_sem=trecv.at[side, 0],
                    device_id=(t, to), device_id_type=MESH).wait_send()


def solution(mesh):
    spaces = mesh.shape["space"]
    constants = tables()
    place = positions()

    def local(fine, coarse, w_query, w_key, w_value, w_out, conv_first, conv_second):
        anywhere = pl.BlockSpec(memory_space=pl.ANY)
        dma = pltpu.SemaphoreType.DMA
        shape = (FL, RL, W, C)
        mats = jnp.asarray(constants)
        moved = pl.pallas_call(
            lambda *refs: kernel(spaces, *refs),
            out_shape=pltpu.VMEM(shape, BF),
            in_specs=[anywhere] * 10,
            out_specs=pl.BlockSpec(memory_space=pltpu.VMEM),
            scratch_shapes=[
                pltpu.VMEM(shape, BF),
                pltpu.VMEM((FL, 2, 128, C), BF),
                pltpu.VMEM((4, C, C), BF),
                pltpu.VMEM((10, 256, 256), BF),
                pltpu.VMEM((8, 1, C), F32),
                pltpu.VMEM((3, 3, C, C), BF),
                pltpu.VMEM((3, 3, C, C), BF),
                pltpu.VMEM((C, C), BF),
                pltpu.VMEM((C, 2 * C), BF),
                pltpu.VMEM((C, C), BF),
                pltpu.VMEM((2 * FL, RL, W, C), BF),
                pltpu.VMEM(shape, BF),
                pltpu.VMEM((RL, FL, W, C), BF),
                pltpu.VMEM((RL, 2 * FL, W, C), BF),
                pltpu.VMEM((RL, 2 * FL, W, C), BF),
                pltpu.VMEM((2 * W, C), BF),
                pltpu.VMEM((FL, RL + 2, W + 32, C), BF),
                pltpu.VMEM((FL, RL + 2, W + 32, C), BF),
                pltpu.VMEM((FL, 2, W, C), F32),
                pltpu.VMEM((2, FL, W, C), BF),
                pltpu.VMEM((2, FL, W, C), BF),
                dma((7,)),
                dma((RL,)),
                dma,
                dma((6,)),
                dma((2,)),
                dma((2, FL, 2)),
                dma((2,)),
                dma((2, FL)),
                pltpu.SemaphoreType.REGULAR,
                pltpu.SemaphoreType.REGULAR,
            ],
            compiler_params=pltpu.CompilerParams(
                collective_id=0, has_side_effects=True, vmem_limit_bytes=60 * 1024 * 1024),
            name="fused",
        )(fine, coarse, w_query, w_key, w_value, w_out, conv_first, conv_second, mats, jnp.asarray(place))
        def emit(x, o, sem):
            for f in range(FL):
                for r in range(0, RL, 2):
                    pltpu.make_async_copy(x.at[f, pl.ds(r, 2)], o.at[f, pl.ds(r, 2)], sem).start()
            pltpu.make_async_copy(x, o, sem).wait()

        return pl.pallas_call(
            emit,
            out_shape=jax.ShapeDtypeStruct(shape, BF),
            in_specs=[pl.BlockSpec(memory_space=pltpu.VMEM)],
            out_specs=anywhere,
            scratch_shapes=[dma],
            name="emit",
        )(pltpu.with_memory_space_constraint(moved, pltpu.VMEM))

    return jax.shard_map(
        local,
        mesh=mesh,
        in_specs=(P("tm", "space", None, None), P("tm", "space", None, None), P(), P(), P(), P(), P(), P()),
        out_specs=P("tm", "space", None, None),
        check_vma=False,
    )
```

```python
import numpy as np
import jax
import jax.numpy as jnp
from jax import lax
from jax.experimental import pallas as pl
from jax.experimental.pallas import tpu as pltpu
from jax.sharding import PartitionSpec as P

HEADS = 8
C = 256
W = 256
FL = 4
RL = 4
BF = jnp.bfloat16
F32 = jnp.float32
MESH = pl.DeviceIdType.MESH


def tables():
    at = np.arange(256)
    col_of = (at % 16) * 16 + at // 16
    columns = np.zeros((256, 256), np.float32)
    columns[at, col_of] = 1.0
    channel = np.zeros((256, 256), np.float32)
    channel[at, (at % 32) * 8 + at // 32] = 1.0
    same = (at[:, None] // 128 == at[None, :] // 128) & (at[:, None] % 8 == at[None, :] % 8)
    heads = same.astype(np.float32)
    widen = np.zeros((256, 128), np.float32)
    for col in range(256):
        half = col // 2
        other = max(half - 1, 0) if col % 2 == 0 else min(half + 1, 127)
        widen[col, half] += 0.75
        widen[col, other] += 0.25
    widen = widen[col_of]
    none = np.zeros_like(widen)

    def pair(first, second):
        return np.concatenate([first * widen, second * widen], axis=1)

    stack = [columns, channel, channel.T, heads, pair(0.75, 0), pair(0.75, 0.25), pair(0.25, 0.75), pair(0, 0.75), pair(0.25, 0), pair(0, 0.25)]
    return np.stack(stack).astype(jnp.bfloat16)


def positions():
    half = C // 2
    inverse = np.exp(-np.log(10000.0) * 2.0 * np.arange(half) / C)
    angles = np.arange(8)[:, None] * inverse[None, :]
    return np.concatenate([np.sin(angles), np.cos(angles)], axis=1).astype(np.float32)[:, None, :]


def taps(ref, lead, first, rows):
    parts = []
    for dy in range(3):
        for dx in range(3):
            parts.append(ref[lead, first + dy : first + dy + rows, 16 * dx : 16 * dx + 256, :].reshape(rows * 256, C))
    return jnp.concatenate(parts, axis=1)


def pads(ref, lead, row):
    index = lax.broadcasted_iota(jnp.int32, (16, C), 0)
    last = ref[lead, row, 256:272, :].astype(F32)
    before = jnp.where(index == 0, 0.0, pltpu.roll(last, 1, axis=0))
    ref[lead, row, 0:16, :] = before.astype(BF)
    leading = ref[lead, row, 16:32, :].astype(F32)
    after = jnp.where(index == 15, 0.0, pltpu.roll(leading, 15, axis=0))
    ref[lead, row, 272:288, :] = after.astype(BF)


def kernel(
    spaces,
    fine_hbm, coarse_hbm, wq_hbm, wk_hbm, wv_hbm, wo_hbm, c1_hbm, c2_hbm, mats_hbm, pos_hbm,
    ob,
    fin, cb, raw, mats, pos, cw1, cw2,
    wqp, wkv, wop, nbuf, fp, qs, kb, vb, att, xp, yp, acc, psend, precv,
    load_sem, row_sem, nsend, nrecv, xsend, xrecv, tsend, trecv, near_sem, far_sem,
):
    t = lax.axis_index("tm")
    s = lax.axis_index("space")
    has_up = s > 0
    has_down = s < spaces - 1

    def row_load(r):
        return pltpu.make_async_copy(fine_hbm.at[:, r], fin.at[:, r], row_sem.at[r])

    loads = [
        pltpu.make_async_copy(mats_hbm.at[0], mats.at[0], load_sem.at[0]),
        pltpu.make_async_copy(mats_hbm.at[pl.ds(0, 4)], raw, load_sem.at[1]),
        pltpu.make_async_copy(pos_hbm, pos, load_sem.at[2]),
        pltpu.make_async_copy(mats_hbm.at[pl.ds(1, 2)], mats.at[pl.ds(1, 2)], load_sem.at[3]),
        pltpu.make_async_copy(coarse_hbm, cb, load_sem.at[4]),
        pltpu.make_async_copy(c1_hbm, cw1, load_sem.at[5]),
        pltpu.make_async_copy(c2_hbm, cw2, load_sem.at[6]),
        pltpu.make_async_copy(mats_hbm.at[pl.ds(3, 7)], mats.at[pl.ds(3, 7)], load_sem.at[7]),
    ]
    for r in (3, 0):
        for f in range(FL):
            pltpu.make_async_copy(fine_hbm.at[f, r], fin.at[f, r], row_sem.at[r]).start()
    loads[0].start()
    loads[2].start()
    for k, weight in enumerate((wq_hbm, wk_hbm, wv_hbm, wo_hbm)):
        pltpu.make_async_copy(weight, raw.at[k], load_sem.at[1]).start()
    loads[3].start()

    barrier = pltpu.get_barrier_semaphore()

    @pl.when(t == 1)
    def _():
        pl.semaphore_signal(barrier, inc=1, device_id=(1 - t, s), device_id_type=MESH)


    @pl.when(t == 0)
    def _():
        pl.semaphore_wait(barrier, 1)
        pl.semaphore_signal(near_sem, inc=1, device_id=(1 - t, s), device_id_type=MESH)

    @pl.when(t == 1)
    def _():
        pl.semaphore_wait(near_sem, 1)

    @pl.when(jnp.logical_and(t == 1, has_up))
    def _():
        pl.semaphore_signal(barrier, inc=1, device_id=(t, s - 1), device_id_type=MESH)

    @pl.when(jnp.logical_and(t == 1, has_down))
    def _():
        pl.semaphore_signal(barrier, inc=1, device_id=(t, s + 1), device_id_type=MESH)

    zero_row = jnp.zeros((FL, 288, C), BF)

    @pl.when(jnp.logical_not(has_up))
    def _():
        xp[:, 0] = zero_row

    @pl.when(jnp.logical_not(has_down))
    def _():
        xp[:, 5] = zero_row

    def norm_copy(k):
        r = (0, 3, 0, 3, 1, 2)[k]
        px = pl.ds((0, 0, 128, 128, 0, 0)[k], 128 if k < 4 else 256)
        return pltpu.make_async_remote_copy(
            src_ref=nbuf.at[pl.ds(0, FL), r, px], dst_ref=nbuf.at[pl.ds(FL, FL), r, px],
            send_sem=nsend, recv_sem=nrecv.at[k],
            device_id=(1 - t, s), device_id_type=MESH)

    def normalize(units, start, count):
        px = slice(start, start + count)
        placed = [jnp.dot(mats[0, px], fin[f, r], preferred_element_type=F32) for f, r in units]
        for (f, r), moved in zip(units, placed):
            fp[f, r, px] = moved.astype(BF)
            hidden = moved + pos[t * FL + f]
            center = hidden - jnp.mean(hidden, axis=-1, keepdims=True)
            spread = jnp.mean(center * center, axis=-1, keepdims=True)
            nbuf[f, r, px] = (center * lax.rsqrt(spread + 1e-05)).astype(BF)

    def edge_copy(a, up, h):
        row, slot, to = (1, 5, s - 1) if up else (4, 0, s + 1)
        side = 0 if up else 1
        px = pl.ds(16 + 128 * h, 128)
        return pltpu.make_async_remote_copy(
            src_ref=xp.at[a, row, px], dst_ref=xp.at[a, slot, px],
            send_sem=xsend.at[side], recv_sem=xrecv.at[side, a, h],
            device_id=(t, to), device_id_type=MESH)

    def part_copy(a, up):
        side = 0 if up else 1
        to = s - 1 if up else s + 1
        return pltpu.make_async_remote_copy(
            src_ref=psend.at[side, a], dst_ref=precv.at[side, a],
            send_sem=tsend.at[side], recv_sem=trecv.at[side, a],
            device_id=(t, to), device_id_type=MESH)

    factor = float(np.log2(np.e) / np.sqrt(32.0))

    def project(rows, frames, own, start, count):
        px = slice(start, start + count)
        units = [(b, r) for b in frames for r in rows]
        stacked = jnp.concatenate([nbuf[b, r, px] for b, r in units], axis=0)
        both = jnp.dot(stacked, wkv[...], preferred_element_type=F32)
        if own:
            query = jnp.dot(stacked, wqp[...], preferred_element_type=F32)
        for i, (b, r) in enumerate(units):
            at = slice(count * i, count * i + count)
            kb[r, b, px] = both[at, 0:256].astype(BF)
            vb[r, b, px] = both[at, 256:512].astype(BF)
            if own:
                qs[r, b, px] = (query[at] * factor).astype(BF)

    def weigh(a, r, start, into):
        px = slice(start, start + 64)
        out = slice(into, into + 64)
        q = qs[r, a, px]
        lhs = []
        for pair in range(4):
            halves = []
            for b in (2 * pair, 2 * pair + 1):
                product = q * kb[r, b, px]
                halves.append(product[:, 0:128] + product[:, 128:256])
            lhs.append(jnp.concatenate(halves, axis=1))
        both = jnp.dot(jnp.concatenate(lhs, axis=0), mats[3], preferred_element_type=F32)
        scores = []
        for b in range(8):
            at = 64 * (b // 2)
            scores.append(both[at : at + 64, 128 * (b % 2) : 128 * (b % 2) + 128])
        largest = scores[0]
        for entry in scores[1:]:
            largest = jnp.maximum(largest, entry)
        powers = [jnp.exp2(entry - largest) for entry in scores]
        total = powers[0]
        for entry in powers[1:]:
            total = total + entry
        inverse = 1.0 / total
        low, high = [], []
        for b in range(8):
            weight = powers[b].astype(BF)
            value = vb[r, b, px]
            low.append(weight * value[:, 0:128])
            high.append(weight * value[:, 128:256])
        while len(low) > 1:
            low = [low[j] + low[j + 1] for j in range(0, len(low), 2)]
            high = [high[j] + high[j + 1] for j in range(0, len(high), 2)]
        att[out, 0:128] = (low[0].astype(F32) * inverse).astype(BF)
        att[out, 128:256] = (high[0].astype(F32) * inverse).astype(BF)

    def attend(units, count, beside=()):
        beside = list(beside)
        into = 0
        for a, r, start in units:
            for px in range(start, start + count, 64):
                weigh(a, r, px, into)
                into += 64
                if into % 128 == 0 and beside:
                    beside.pop(0)()
        for run in beside:
            run()
        branch = jnp.dot(att[0:into], wop[...], preferred_element_type=F32)
        for i, (a, r, start) in enumerate(units):
            px = slice(start, start + count)
            moved = (fp[a, r, px].astype(F32) + branch[count * i : count * i + count]).astype(BF)
            fp[a, r, px] = moved
            xp[a, r + 1, 16 + start : 16 + start + count, :] = jnp.maximum(moved, jnp.zeros_like(moved))

    def send_up(a, h):
        @pl.when(has_up)
        def _():
            edge_copy(a, True, h).start()

    def send_down(a, h):
        @pl.when(has_down)
        def _():
            edge_copy(a, False, h).start()

    def send_edges(a, h):
        send_down(a, h)
        send_up(a, h)

    def wait_norms(ks):
        with jax.named_scope("norm_wait"):
            for k in ks:
                norm_copy(k).wait_recv()

    def first_wait(a):
        @pl.when(has_up)
        def _():
            with jax.named_scope("edge_wait_up"):
                for h in range(2):
                    edge_copy(a, False, h).wait_recv()

        @pl.when(has_down)
        def _():
            with jax.named_scope("edge_wait_down"):
                for h in range(2):
                    edge_copy(a, True, h).wait_recv()

    def first_rows(a, rows):
        weight = cw1[...].reshape(9 * C, C)

        def run(y):
            result = jnp.dot(taps(xp, a, y, 1), weight, preferred_element_type=F32)
            yp[a, 1 + y, 16:272, :] = jnp.maximum(result, 0.0).astype(BF)

        return [lambda y=y: run(y) for y in rows]

    def first_end(a):
        for r in range(1, 5):
            pads(yp, a, r)
        near = cb[a].reshape(256, C)
        parts = []
        for side, row, dy in ((0, 1, 2), (1, 4, 0)):
            lhs = jnp.concatenate([yp[a, row, 16 * dx : 16 * dx + 256, :] for dx in range(3)], axis=1)
            parts.append(jnp.dot(lhs, cw2[dy].reshape(3 * C, C), preferred_element_type=F32))
        for side in (0, 1):
            parts[side] = parts[side] + jnp.dot(mats[8 + side], near, preferred_element_type=F32)
        for side in (0, 1):
            psend[side, a] = parts[side].astype(BF)

    def send_parts(a):
        @pl.when(has_up)
        def _():
            part_copy(a, True).start()

        @pl.when(has_down)
        def _():
            part_copy(a, False).start()

    with jax.named_scope("load_wait"):
        loads[0].wait()
        loads[2].wait()
        row_load(0).wait()
        row_load(3).wait()
    loads[7].start()
    row_load(1).start()
    row_load(2).start()
    for copy in loads[4:7]:
        copy.start()
    edge_units = [(f, r) for f in range(FL) for r in (0, 3)]
    with jax.named_scope("norm03"):
        normalize(edge_units, 0, 128)
    norm_copy(1).start()
    norm_copy(0).start()
    with jax.named_scope("weights"):
        loads[1].wait()
        loads[3].wait()
        wqp[...] = jnp.dot(raw[0], mats[1], preferred_element_type=F32).astype(BF)
        wkv[:, 0:256] = jnp.dot(raw[1], mats[1], preferred_element_type=F32).astype(BF)
        wkv[:, 256:512] = jnp.dot(raw[2], mats[1], preferred_element_type=F32).astype(BF)
        wop[...] = jnp.dot(mats[2], raw[3], preferred_element_type=F32).astype(BF)
    with jax.named_scope("keys03"):
        project((0, 3), range(0, 4), True, 0, 128)
    with jax.named_scope("norm03b"):
        normalize(edge_units, 128, 128)
    norm_copy(3).start()
    norm_copy(2).start()

    def edge_pair(k, h, beside):
        frames = (2 * k, 2 * k + 1)
        attend([(a, r, 128 * h) for a in frames for r in (0, 3)], 128, beside)
        for a in frames:
            send_edges(a, h)

    @pl.when(t == 1)
    def _():
        pl.semaphore_wait(barrier, has_up.astype(jnp.int32) + has_down.astype(jnp.int32))
        pl.semaphore_signal(far_sem, inc=1, device_id=(1 - t, s), device_id_type=MESH)

    with jax.named_scope("attend03"):
        loads[7].wait()
        wait_norms((1,))
        project((3,), range(4, 8), False, 0, 128)
        attend([(0, 3, 0)], 128)
        with jax.named_scope("meet"):
            @pl.when(t == 0)
            def _():
                pl.semaphore_wait(far_sem, 1)

        send_down(0, 0)
        wait_norms((0,))
        project((0,), range(4, 8), False, 0, 128)
        attend([(0, 0, 0)], 128)
        send_up(0, 0)
        attend([(1, 0, 0), (1, 3, 0)], 128, [lambda k=k: project((0, 3), (2 * k, 2 * k + 1), True, 128, 128) for k in range(2)])
        send_edges(1, 0)
    def inner_norm(pair, carry):
        normalize([(2 * pair + k, r) for k in range(2) for r in (1, 2)], 0, 256)
        return carry

    wait_norms((2, 3))
    with jax.named_scope("attend03b"):
        project((0, 3), range(4, 8), False, 128, 128)
        edge_pair(0, 1, [])
    with jax.named_scope("norm12"):
        row_load(1).wait()
        row_load(2).wait()
        lax.fori_loop(0, 2, inner_norm, 0)
    norm_copy(4).start()
    norm_copy(5).start()
    with jax.named_scope("attend03c"):
        edge_pair(1, 0, [lambda b=b: project((1, 2), (b,), True, 0, 256) for b in range(0, 4)])
    with jax.named_scope("attend03d"):
        edge_pair(1, 1, [])
    wait_norms((4, 5))
    with jax.named_scope("keys12b"):
        for b in range(4, 8, 2):
            project((1, 2), (b, b + 1), False, 0, 256)
    with jax.named_scope("attend12"):
        attend([(0, 1, 0), (0, 2, 0)], 256)
    for copy in loads[4:7]:
        copy.wait()

    def mixed_step(a, carry):
        for r in range(1, 5):
            pads(xp, a, r)
        attend([(a + 1, 1, 0), (a + 1, 2, 0)], 256, first_rows(a, (1, 2)))
        first_wait(a)
        outer(a)
        send_parts(a)
        return carry

    def outer(a):
        for r in (0, 5):
            pads(xp, a, r)
        for run in first_rows(a, (0, 3)):
            run()
        first_end(a)

    with jax.named_scope("mixed"):
        lax.fori_loop(0, FL - 1, mixed_step, 0)
    with jax.named_scope("first"):
        for r in range(1, 5):
            pads(xp, FL - 1, r)
        first_wait(FL - 1)
        outer(FL - 1)
        send_parts(FL - 1)
        for run in first_rows(FL - 1, (1, 2)):
            run()
        for r in (2, 3):
            pads(yp, FL - 1, r)

    def second_step(a, carry):
        near = cb[a].reshape(256, C)
        inner = jnp.dot(taps(yp, a, 1, 2), cw2[...].reshape(9 * C, C), preferred_element_type=F32)
        outer = []
        for row, first, dys in ((0, 1, (1, 2)), (3, 3, (0, 1))):
            parts = [yp[a, first + k, 16 * dx : 16 * dx + 256, :] for k in range(2) for dx in range(3)]
            weight = cw2[dys[0] : dys[0] + 2].reshape(6 * C, C)
            outer.append(jnp.dot(jnp.concatenate(parts, axis=1), weight, preferred_element_type=F32))
        up = jnp.dot(mats[4:8].reshape(4 * 256, 256), near, preferred_element_type=F32)
        for row, value in ((1, inner[0:256]), (2, inner[256:512]), (0, outer[0]), (3, outer[1])):
            value = value + up[256 * row : 256 * row + 256] + fp[a, row].astype(F32)
            if row in (1, 2):
                fp[a, row] = value.astype(BF)
            else:
                acc[a, row // 3] = value
        return carry

    with jax.named_scope("second"):
        lax.fori_loop(0, FL, second_step, 0)

    def edge_part(a, side):
        near = cb[a].reshape(256, C)
        precv[1 - side, a] = jnp.dot(mats[8 + side], near, preferred_element_type=F32).astype(BF)

    def last_step(a, carry):
        @pl.when(has_up)
        def _():
            with jax.named_scope("part_wait_up"):
                part_copy(a, False).wait_recv()

        @pl.when(jnp.logical_not(has_up))
        def _():
            edge_part(a, 0)

        @pl.when(has_down)
        def _():
            with jax.named_scope("part_wait_down"):
                part_copy(a, True).wait_recv()

        @pl.when(jnp.logical_not(has_down))
        def _():
            edge_part(a, 1)

        for row, side in ((0, 1), (3, 0)):
            value = (acc[a, row // 3] + precv[side, a].astype(F32)).astype(BF)
            ob[a, row] = jnp.dot(mats[0], value, preferred_element_type=F32).astype(BF)
        return carry

    def restore_step(a, carry):
        for row in (1, 2):
            ob[a, row] = jnp.dot(mats[0], fp[a, row], preferred_element_type=F32).astype(BF)
        return carry

    with jax.named_scope("restore"):
        lax.fori_loop(0, FL, restore_step, 0)
    with jax.named_scope("last"):
        lax.fori_loop(0, FL, last_step, 0)

    with jax.named_scope("drain"):
        pltpu.make_async_remote_copy(
            src_ref=nbuf.at[pl.ds(0, FL)], dst_ref=nbuf.at[pl.ds(FL, FL)], send_sem=nsend, recv_sem=nrecv.at[0],
            device_id=(1 - t, s), device_id_type=MESH).wait_send()
        for side, flag, row, slot, to in ((0, has_up, 1, 5, s - 1), (1, has_down, 4, 0, s + 1)):
            @pl.when(flag)
            def _(side=side, row=row, slot=slot, to=to):
                pltpu.make_async_remote_copy(
                    src_ref=xp.at[:, row, pl.ds(16, 256)], dst_ref=xp.at[:, slot, pl.ds(16, 256)],
                    send_sem=xsend.at[side], recv_sem=xrecv.at[side, 0, 0],
                    device_id=(t, to), device_id_type=MESH).wait_send()
                pltpu.make_async_remote_copy(
                    src_ref=psend.at[side], dst_ref=precv.at[side],
                    send_sem=tsend.at[side], recv_sem=trecv.at[side, 0],
                    device_id=(t, to), device_id_type=MESH).wait_send()


def solution(mesh):
    spaces = mesh.shape["space"]
    constants = tables()
    place = positions()

    def local(fine, coarse, w_query, w_key, w_value, w_out, conv_first, conv_second):
        anywhere = pl.BlockSpec(memory_space=pl.ANY)
        dma = pltpu.SemaphoreType.DMA
        shape = (FL, RL, W, C)
        mats = jnp.asarray(constants)
        moved = pl.pallas_call(
            lambda *refs: kernel(spaces, *refs),
            out_shape=pltpu.VMEM(shape, BF),
            in_specs=[anywhere] * 10,
            out_specs=pl.BlockSpec(memory_space=pltpu.VMEM),
            scratch_shapes=[
                pltpu.VMEM(shape, BF),
                pltpu.VMEM((FL, 2, 128, C), BF),
                pltpu.VMEM((4, C, C), BF),
                pltpu.VMEM((10, 256, 256), BF),
                pltpu.VMEM((8, 1, C), F32),
                pltpu.VMEM((3, 3, C, C), BF),
                pltpu.VMEM((3, 3, C, C), BF),
                pltpu.VMEM((C, C), BF),
                pltpu.VMEM((C, 2 * C), BF),
                pltpu.VMEM((C, C), BF),
                pltpu.VMEM((2 * FL, RL, W, C), BF),
                pltpu.VMEM(shape, BF),
                pltpu.VMEM((RL, FL, W, C), BF),
                pltpu.VMEM((RL, 2 * FL, W, C), BF),
                pltpu.VMEM((RL, 2 * FL, W, C), BF),
                pltpu.VMEM((2 * W, C), BF),
                pltpu.VMEM((FL, RL + 2, W + 32, C), BF),
                pltpu.VMEM((FL, RL + 2, W + 32, C), BF),
                pltpu.VMEM((FL, 2, W, C), F32),
                pltpu.VMEM((2, FL, W, C), BF),
                pltpu.VMEM((2, FL, W, C), BF),
                dma((8,)),
                dma((RL,)),
                dma,
                dma((6,)),
                dma((2,)),
                dma((2, FL, 2)),
                dma((2,)),
                dma((2, FL)),
                pltpu.SemaphoreType.REGULAR,
                pltpu.SemaphoreType.REGULAR,
            ],
            compiler_params=pltpu.CompilerParams(
                collective_id=0, has_side_effects=True, vmem_limit_bytes=60 * 1024 * 1024),
            name="fused",
        )(fine, coarse, w_query, w_key, w_value, w_out, conv_first, conv_second, mats, jnp.asarray(place))
        def emit(x, o, sem):
            for f in range(FL):
                for r in range(0, RL, 2):
                    pltpu.make_async_copy(x.at[f, pl.ds(r, 2)], o.at[f, pl.ds(r, 2)], sem).start()
            pltpu.make_async_copy(x, o, sem).wait()

        return pl.pallas_call(
            emit,
            out_shape=jax.ShapeDtypeStruct(shape, BF),
            in_specs=[pl.BlockSpec(memory_space=pltpu.VMEM)],
            out_specs=anywhere,
            scratch_shapes=[dma],
            name="emit",
        )(pltpu.with_memory_space_constraint(moved, pltpu.VMEM))

    return jax.shard_map(
        local,
        mesh=mesh,
        in_specs=(P("tm", "space", None, None), P("tm", "space", None, None), P(), P(), P(), P(), P(), P()),
        out_specs=P("tm", "space", None, None),
        check_vma=False,
    )
```

```python
import numpy as np
import jax
import jax.numpy as jnp
from jax import lax
from jax.experimental import pallas as pl
from jax.experimental.pallas import tpu as pltpu
from jax.sharding import PartitionSpec as P

HEADS = 8
C = 256
W = 256
FL = 4
RL = 4
BF = jnp.bfloat16
F32 = jnp.float32
MESH = pl.DeviceIdType.MESH


def tables():
    at = np.arange(256)
    col_of = (at % 16) * 16 + at // 16
    columns = np.zeros((256, 256), np.float32)
    columns[at, col_of] = 1.0
    channel = np.zeros((256, 256), np.float32)
    channel[at, (at % 32) * 8 + at // 32] = 1.0
    same = (at[:, None] // 128 == at[None, :] // 128) & (at[:, None] % 8 == at[None, :] % 8)
    heads = same.astype(np.float32)
    widen = np.zeros((256, 128), np.float32)
    for col in range(256):
        half = col // 2
        other = max(half - 1, 0) if col % 2 == 0 else min(half + 1, 127)
        widen[col, half] += 0.75
        widen[col, other] += 0.25
    widen = widen[col_of]
    none = np.zeros_like(widen)

    def pair(first, second):
        return np.concatenate([first * widen, second * widen], axis=1)

    stack = [columns, channel, channel.T, heads, pair(0.75, 0), pair(0.75, 0.25), pair(0.25, 0.75), pair(0, 0.75), pair(0.25, 0), pair(0, 0.25)]
    return np.stack(stack).astype(jnp.bfloat16)


def positions():
    half = C // 2
    inverse = np.exp(-np.log(10000.0) * 2.0 * np.arange(half) / C)
    angles = np.arange(8)[:, None] * inverse[None, :]
    return np.concatenate([np.sin(angles), np.cos(angles)], axis=1).astype(np.float32)[:, None, :]


def taps(ref, lead, first, rows):
    parts = []
    for dy in range(3):
        for dx in range(3):
            parts.append(ref[lead, first + dy : first + dy + rows, 16 * dx : 16 * dx + 256, :].reshape(rows * 256, C))
    return jnp.concatenate(parts, axis=1)


def pads(ref, lead, row):
    index = lax.broadcasted_iota(jnp.int32, (16, C), 0)
    last = ref[lead, row, 256:272, :].astype(F32)
    before = jnp.where(index == 0, 0.0, pltpu.roll(last, 1, axis=0))
    ref[lead, row, 0:16, :] = before.astype(BF)
    leading = ref[lead, row, 16:32, :].astype(F32)
    after = jnp.where(index == 15, 0.0, pltpu.roll(leading, 15, axis=0))
    ref[lead, row, 272:288, :] = after.astype(BF)


def kernel(
    spaces,
    fine_hbm, coarse_hbm, wq_hbm, wk_hbm, wv_hbm, wo_hbm, c1_hbm, c2_hbm, mats_hbm, pos_hbm,
    ob,
    fin, cb, raw, mats, pos, cw1, cw2,
    wqp, wkv, wop, nbuf, fp, qs, kb, vb, att, xp, yp, acc, psend, precv,
    load_sem, row_sem, nsend, nrecv, xsend, xrecv, tsend, trecv, near_sem, far_sem,
):
    t = lax.axis_index("tm")
    s = lax.axis_index("space")
    has_up = s > 0
    has_down = s < spaces - 1

    def rows_load(k):
        return pltpu.make_async_copy(fine_hbm.at[:, pl.ds(1, 2)], fin.at[:, pl.ds(1, 2)], row_sem.at[k])

    loads = [
        pltpu.make_async_copy(mats_hbm.at[0], mats.at[0], load_sem.at[0]),
        pltpu.make_async_copy(mats_hbm.at[pl.ds(0, 4)], raw, load_sem.at[1]),
        pltpu.make_async_copy(pos_hbm, pos, load_sem.at[2]),
        pltpu.make_async_copy(mats_hbm.at[pl.ds(1, 2)], mats.at[pl.ds(1, 2)], load_sem.at[3]),
        pltpu.make_async_copy(coarse_hbm, cb, load_sem.at[4]),
        pltpu.make_async_copy(c1_hbm, cw1, load_sem.at[5]),
        pltpu.make_async_copy(c2_hbm, cw2, load_sem.at[6]),
        pltpu.make_async_copy(mats_hbm.at[pl.ds(3, 7)], mats.at[pl.ds(3, 7)], load_sem.at[7]),
    ]
    for r in (3, 0):
        for f in range(FL):
            pltpu.make_async_copy(fine_hbm.at[f, r], fin.at[f, r], row_sem.at[0]).start()
    loads[0].start()
    loads[2].start()
    for k, weight in enumerate((wq_hbm, wk_hbm, wv_hbm, wo_hbm)):
        pltpu.make_async_copy(weight, raw.at[k], load_sem.at[1]).start()
    loads[3].start()

    barrier = pltpu.get_barrier_semaphore()

    @pl.when(t == 1)
    def _():
        pl.semaphore_signal(barrier, inc=1, device_id=(1 - t, s), device_id_type=MESH)


    @pl.when(t == 0)
    def _():
        pl.semaphore_wait(barrier, 1)
        pl.semaphore_signal(near_sem, inc=1, device_id=(1 - t, s), device_id_type=MESH)

    @pl.when(t == 1)
    def _():
        pl.semaphore_wait(near_sem, 1)

    @pl.when(jnp.logical_and(t == 1, has_up))
    def _():
        pl.semaphore_signal(barrier, inc=1, device_id=(t, s - 1), device_id_type=MESH)

    @pl.when(jnp.logical_and(t == 1, has_down))
    def _():
        pl.semaphore_signal(barrier, inc=1, device_id=(t, s + 1), device_id_type=MESH)

    zero_row = jnp.zeros((FL, 288, C), BF)

    @pl.when(jnp.logical_not(has_up))
    def _():
        xp[:, 0] = zero_row

    @pl.when(jnp.logical_not(has_down))
    def _():
        xp[:, 5] = zero_row

    def norm_copy(k):
        r = (0, 3, 0, 3, 1, 2)[k]
        px = pl.ds((0, 0, 128, 128, 0, 0)[k], 128 if k < 4 else 256)
        return pltpu.make_async_remote_copy(
            src_ref=nbuf.at[pl.ds(0, FL), r, px], dst_ref=nbuf.at[pl.ds(FL, FL), r, px],
            send_sem=nsend, recv_sem=nrecv.at[k],
            device_id=(1 - t, s), device_id_type=MESH)

    def normalize(units, start, count):
        px = slice(start, start + count)
        placed = [jnp.dot(mats[0, px], fin[f, r], preferred_element_type=F32) for f, r in units]
        for (f, r), moved in zip(units, placed):
            fp[f, r, px] = moved.astype(BF)
            hidden = moved + pos[t * FL + f]
            center = hidden - jnp.mean(hidden, axis=-1, keepdims=True)
            spread = jnp.mean(center * center, axis=-1, keepdims=True)
            nbuf[f, r, px] = (center * lax.rsqrt(spread + 1e-05)).astype(BF)

    def edge_copy(a, up, h):
        row, slot, to = (1, 5, s - 1) if up else (4, 0, s + 1)
        side = 0 if up else 1
        px = pl.ds(16 + 128 * h, 128)
        return pltpu.make_async_remote_copy(
            src_ref=xp.at[a, row, px], dst_ref=xp.at[a, slot, px],
            send_sem=xsend.at[side], recv_sem=xrecv.at[side, a],
            device_id=(t, to), device_id_type=MESH)

    def part_copy(a, up):
        side = 0 if up else 1
        to = s - 1 if up else s + 1
        return pltpu.make_async_remote_copy(
            src_ref=psend.at[side, a], dst_ref=precv.at[side, a],
            send_sem=tsend.at[side], recv_sem=trecv.at[side, a],
            device_id=(t, to), device_id_type=MESH)

    factor = float(np.log2(np.e) / np.sqrt(32.0))

    def project(rows, frames, own, start, count):
        px = slice(start, start + count)
        units = [(b, r) for b in frames for r in rows]
        stacked = jnp.concatenate([nbuf[b, r, px] for b, r in units], axis=0)
        both = jnp.dot(stacked, wkv[...], preferred_element_type=F32)
        if own:
            query = jnp.dot(stacked, wqp[...], preferred_element_type=F32)
        for i, (b, r) in enumerate(units):
            at = slice(count * i, count * i + count)
            kb[r, b, px] = both[at, 0:256].astype(BF)
            vb[r, b, px] = both[at, 256:512].astype(BF)
            if own:
                qs[r, b, px] = (query[at] * factor).astype(BF)

    def weigh(a, r, start, into):
        px = slice(start, start + 64)
        out = slice(into, into + 64)
        q = qs[r, a, px]
        lhs = []
        for pair in range(4):
            halves = []
            for b in (2 * pair, 2 * pair + 1):
                product = q * kb[r, b, px]
                halves.append(product[:, 0:128] + product[:, 128:256])
            lhs.append(jnp.concatenate(halves, axis=1))
        both = jnp.dot(jnp.concatenate(lhs, axis=0), mats[3], preferred_element_type=F32)
        scores = []
        for b in range(8):
            at = 64 * (b // 2)
            scores.append(both[at : at + 64, 128 * (b % 2) : 128 * (b % 2) + 128])
        largest = scores[0]
        for entry in scores[1:]:
            largest = jnp.maximum(largest, entry)
        powers = [jnp.exp2(entry - largest) for entry in scores]
        total = powers[0]
        for entry in powers[1:]:
            total = total + entry
        inverse = 1.0 / total
        low, high = [], []
        for b in range(8):
            weight = powers[b].astype(BF)
            value = vb[r, b, px]
            low.append(weight * value[:, 0:128])
            high.append(weight * value[:, 128:256])
        while len(low) > 1:
            low = [low[j] + low[j + 1] for j in range(0, len(low), 2)]
            high = [high[j] + high[j + 1] for j in range(0, len(high), 2)]
        att[out, 0:128] = (low[0].astype(F32) * inverse).astype(BF)
        att[out, 128:256] = (high[0].astype(F32) * inverse).astype(BF)

    def attend(units, count, beside=()):
        beside = list(beside)
        into = 0
        for a, r, start in units:
            for px in range(start, start + count, 64):
                weigh(a, r, px, into)
                into += 64
                if into % 128 == 0 and beside:
                    beside.pop(0)()
        for run in beside:
            run()
        branch = jnp.dot(att[0:into], wop[...], preferred_element_type=F32)
        for i, (a, r, start) in enumerate(units):
            px = slice(start, start + count)
            moved = (fp[a, r, px].astype(F32) + branch[count * i : count * i + count]).astype(BF)
            fp[a, r, px] = moved
            xp[a, r + 1, 16 + start : 16 + start + count, :] = jnp.maximum(moved, jnp.zeros_like(moved))

    def send_up(a, h):
        @pl.when(has_up)
        def _():
            edge_copy(a, True, h).start()

    def send_down(a, h):
        @pl.when(has_down)
        def _():
            edge_copy(a, False, h).start()

    def send_edges(a, h):
        send_down(a, h)
        send_up(a, h)

    def wait_norms(ks):
        with jax.named_scope("norm_wait"):
            for k in ks:
                norm_copy(k).wait_recv()

    def edge_whole(a, up):
        row, slot, to = (1, 5, s - 1) if up else (4, 0, s + 1)
        side = 0 if up else 1
        return pltpu.make_async_remote_copy(
            src_ref=xp.at[a, row, pl.ds(16, 256)], dst_ref=xp.at[a, slot, pl.ds(16, 256)],
            send_sem=xsend.at[side], recv_sem=xrecv.at[side, a],
            device_id=(t, to), device_id_type=MESH)

    def first_wait(a):
        @pl.when(has_up)
        def _():
            with jax.named_scope("edge_wait_up"):
                edge_whole(a, False).wait_recv()

        @pl.when(has_down)
        def _():
            with jax.named_scope("edge_wait_down"):
                edge_whole(a, True).wait_recv()

    def first_rows(a, rows):
        weight = cw1[...].reshape(9 * C, C)

        def run(y):
            result = jnp.dot(taps(xp, a, y, 1), weight, preferred_element_type=F32)
            yp[a, 1 + y, 16:272, :] = jnp.maximum(result, 0.0).astype(BF)

        return [lambda y=y: run(y) for y in rows]

    def first_end(a):
        for r in range(1, 5):
            pads(yp, a, r)
        near = cb[a].reshape(256, C)
        parts = []
        for side, row, dy in ((0, 1, 2), (1, 4, 0)):
            lhs = jnp.concatenate([yp[a, row, 16 * dx : 16 * dx + 256, :] for dx in range(3)], axis=1)
            parts.append(jnp.dot(lhs, cw2[dy].reshape(3 * C, C), preferred_element_type=F32))
        for side in (0, 1):
            parts[side] = parts[side] + jnp.dot(mats[8 + side], near, preferred_element_type=F32)
        for side in (0, 1):
            psend[side, a] = parts[side].astype(BF)

    def send_parts(a):
        @pl.when(has_up)
        def _():
            part_copy(a, True).start()

        @pl.when(has_down)
        def _():
            part_copy(a, False).start()

    with jax.named_scope("load_wait"):
        loads[0].wait()
        loads[2].wait()
        rows_load(0).wait()
    loads[7].start()
    rows_load(1).start()
    for copy in loads[4:7]:
        copy.start()
    edge_units = [(f, r) for f in range(FL) for r in (0, 3)]
    with jax.named_scope("norm03"):
        normalize(edge_units, 0, 128)
    norm_copy(1).start()
    norm_copy(0).start()
    with jax.named_scope("weights"):
        loads[1].wait()
        loads[3].wait()
        wqp[...] = jnp.dot(raw[0], mats[1], preferred_element_type=F32).astype(BF)
        wkv[:, 0:256] = jnp.dot(raw[1], mats[1], preferred_element_type=F32).astype(BF)
        wkv[:, 256:512] = jnp.dot(raw[2], mats[1], preferred_element_type=F32).astype(BF)
        wop[...] = jnp.dot(mats[2], raw[3], preferred_element_type=F32).astype(BF)
    with jax.named_scope("keys03"):
        project((0, 3), range(0, 4), True, 0, 128)
    with jax.named_scope("norm03b"):
        normalize(edge_units, 128, 128)
    norm_copy(3).start()
    norm_copy(2).start()

    def edge_pair(k, h, beside):
        frames = (2 * k, 2 * k + 1)
        attend([(a, r, 128 * h) for a in frames for r in (0, 3)], 128, beside)
        for a in frames:
            send_edges(a, h)

    @pl.when(t == 1)
    def _():
        pl.semaphore_wait(barrier, has_up.astype(jnp.int32) + has_down.astype(jnp.int32))
        pl.semaphore_signal(far_sem, inc=1, device_id=(1 - t, s), device_id_type=MESH)

    with jax.named_scope("attend03"):
        loads[7].wait()
        wait_norms((1,))
        project((3,), range(4, 8), False, 0, 128)
        attend([(0, 3, 0)], 128)
        with jax.named_scope("meet"):
            @pl.when(t == 0)
            def _():
                pl.semaphore_wait(far_sem, 1)

        send_down(0, 0)
        wait_norms((0,))
        project((0,), range(4, 8), False, 0, 128)
        attend([(0, 0, 0)], 128)
        send_up(0, 0)
        attend([(1, 0, 0), (1, 3, 0)], 128, [lambda k=k: project((0, 3), (2 * k, 2 * k + 1), True, 128, 128) for k in range(2)])
        send_edges(1, 0)
    def inner_norm(pair, carry):
        normalize([(2 * pair + k, r) for k in range(2) for r in (1, 2)], 0, 256)
        return carry

    wait_norms((2, 3))
    with jax.named_scope("attend03b"):
        project((0, 3), range(4, 8), False, 128, 128)
        edge_pair(0, 1, [])
    with jax.named_scope("norm12"):
        rows_load(1).wait()
        lax.fori_loop(0, 2, inner_norm, 0)
    norm_copy(4).start()
    norm_copy(5).start()
    with jax.named_scope("attend03c"):
        edge_pair(1, 0, [lambda b=b: project((1, 2), (b,), True, 0, 256) for b in range(0, 4)])
    with jax.named_scope("attend03d"):
        edge_pair(1, 1, [])
    wait_norms((4, 5))
    with jax.named_scope("keys12b"):
        for b in range(4, 8, 2):
            project((1, 2), (b, b + 1), False, 0, 256)
    with jax.named_scope("attend12"):
        attend([(0, 1, 0), (0, 2, 0)], 256)
    for copy in loads[4:7]:
        copy.wait()

    def mixed_step(a, carry):
        for r in range(1, 5):
            pads(xp, a, r)
        attend([(a + 1, 1, 0), (a + 1, 2, 0)], 256, first_rows(a, (1, 2)))
        first_wait(a)
        outer(a)
        send_parts(a)
        return carry

    def outer(a):
        for r in (0, 5):
            pads(xp, a, r)
        for run in first_rows(a, (0, 3)):
            run()
        first_end(a)

    with jax.named_scope("mixed"):
        lax.fori_loop(0, FL - 1, mixed_step, 0)
    with jax.named_scope("first"):
        for r in range(1, 5):
            pads(xp, FL - 1, r)
        first_wait(FL - 1)
        outer(FL - 1)
        send_parts(FL - 1)
        for run in first_rows(FL - 1, (1, 2)):
            run()
        for r in (2, 3):
            pads(yp, FL - 1, r)

    def second_step(a, carry):
        near = cb[a].reshape(256, C)
        inner = jnp.dot(taps(yp, a, 1, 2), cw2[...].reshape(9 * C, C), preferred_element_type=F32)
        outer = []
        for row, first, dys in ((0, 1, (1, 2)), (3, 3, (0, 1))):
            parts = [yp[a, first + k, 16 * dx : 16 * dx + 256, :] for k in range(2) for dx in range(3)]
            weight = cw2[dys[0] : dys[0] + 2].reshape(6 * C, C)
            outer.append(jnp.dot(jnp.concatenate(parts, axis=1), weight, preferred_element_type=F32))
        up = jnp.dot(mats[4:8].reshape(4 * 256, 256), near, preferred_element_type=F32)
        for row, value in ((1, inner[0:256]), (2, inner[256:512]), (0, outer[0]), (3, outer[1])):
            value = value + up[256 * row : 256 * row + 256] + fp[a, row].astype(F32)
            if row in (1, 2):
                fp[a, row] = value.astype(BF)
            else:
                acc[a, row // 3] = value
        return carry

    with jax.named_scope("second"):
        lax.fori_loop(0, FL, second_step, 0)

    def edge_part(a, side):
        near = cb[a].reshape(256, C)
        precv[1 - side, a] = jnp.dot(mats[8 + side], near, preferred_element_type=F32).astype(BF)

    def last_row(a, k):
        value = (acc[a, k] + precv[1 - k, a].astype(F32)).astype(BF)
        ob[a, 3 * k] = jnp.dot(mats[0], value, preferred_element_type=F32).astype(BF)

    def last_step(a, carry):
        @pl.when(has_down)
        def _():
            with jax.named_scope("part_wait_down"):
                part_copy(a, True).wait_recv()

        @pl.when(jnp.logical_not(has_down))
        def _():
            edge_part(a, 1)

        last_row(a, 1)

        @pl.when(has_up)
        def _():
            with jax.named_scope("part_wait_up"):
                part_copy(a, False).wait_recv()

        @pl.when(jnp.logical_not(has_up))
        def _():
            edge_part(a, 0)

        last_row(a, 0)
        return carry

    def restore_step(a, carry):
        for row in (1, 2):
            ob[a, row] = jnp.dot(mats[0], fp[a, row], preferred_element_type=F32).astype(BF)
        return carry

    with jax.named_scope("restore"):
        lax.fori_loop(0, FL, restore_step, 0)
    with jax.named_scope("last"):
        lax.fori_loop(0, FL, last_step, 0)

    with jax.named_scope("drain"):
        pltpu.make_async_remote_copy(
            src_ref=nbuf.at[pl.ds(0, FL)], dst_ref=nbuf.at[pl.ds(FL, FL)], send_sem=nsend, recv_sem=nrecv.at[0],
            device_id=(1 - t, s), device_id_type=MESH).wait_send()
        for side, flag, row, slot, to in ((0, has_up, 1, 5, s - 1), (1, has_down, 4, 0, s + 1)):
            @pl.when(flag)
            def _(side=side, row=row, slot=slot, to=to):
                pltpu.make_async_remote_copy(
                    src_ref=xp.at[:, row, pl.ds(16, 256)], dst_ref=xp.at[:, slot, pl.ds(16, 256)],
                    send_sem=xsend.at[side], recv_sem=xrecv.at[side, 0],
                    device_id=(t, to), device_id_type=MESH).wait_send()
                pltpu.make_async_remote_copy(
                    src_ref=psend.at[side], dst_ref=precv.at[side],
                    send_sem=tsend.at[side], recv_sem=trecv.at[side, 0],
                    device_id=(t, to), device_id_type=MESH).wait_send()


def solution(mesh):
    spaces = mesh.shape["space"]
    constants = tables()
    place = positions()

    def local(fine, coarse, w_query, w_key, w_value, w_out, conv_first, conv_second):
        anywhere = pl.BlockSpec(memory_space=pl.ANY)
        dma = pltpu.SemaphoreType.DMA
        shape = (FL, RL, W, C)
        mats = jnp.asarray(constants)
        moved = pl.pallas_call(
            lambda *refs: kernel(spaces, *refs),
            out_shape=pltpu.VMEM(shape, BF),
            in_specs=[anywhere] * 10,
            out_specs=pl.BlockSpec(memory_space=pltpu.VMEM),
            scratch_shapes=[
                pltpu.VMEM(shape, BF),
                pltpu.VMEM((FL, 2, 128, C), BF),
                pltpu.VMEM((4, C, C), BF),
                pltpu.VMEM((10, 256, 256), BF),
                pltpu.VMEM((8, 1, C), F32),
                pltpu.VMEM((3, 3, C, C), BF),
                pltpu.VMEM((3, 3, C, C), BF),
                pltpu.VMEM((C, C), BF),
                pltpu.VMEM((C, 2 * C), BF),
                pltpu.VMEM((C, C), BF),
                pltpu.VMEM((2 * FL, RL, W, C), BF),
                pltpu.VMEM(shape, BF),
                pltpu.VMEM((RL, FL, W, C), BF),
                pltpu.VMEM((RL, 2 * FL, W, C), BF),
                pltpu.VMEM((RL, 2 * FL, W, C), BF),
                pltpu.VMEM((2 * W, C), BF),
                pltpu.VMEM((FL, RL + 2, W + 32, C), BF),
                pltpu.VMEM((FL, RL + 2, W + 32, C), BF),
                pltpu.VMEM((FL, 2, W, C), F32),
                pltpu.VMEM((2, FL, W, C), BF),
                pltpu.VMEM((2, FL, W, C), BF),
                dma((8,)),
                dma((2,)),
                dma,
                dma((6,)),
                dma((2,)),
                dma((2, FL)),
                dma((2,)),
                dma((2, FL)),
                pltpu.SemaphoreType.REGULAR,
                pltpu.SemaphoreType.REGULAR,
            ],
            compiler_params=pltpu.CompilerParams(
                collective_id=0, has_side_effects=True, vmem_limit_bytes=60 * 1024 * 1024),
            name="fused",
        )(fine, coarse, w_query, w_key, w_value, w_out, conv_first, conv_second, mats, jnp.asarray(place))
        def emit(x, o, sem):
            for f in range(FL):
                for r in range(0, RL, 2):
                    pltpu.make_async_copy(x.at[f, pl.ds(r, 2)], o.at[f, pl.ds(r, 2)], sem).start()
            pltpu.make_async_copy(x, o, sem).wait()

        return pl.pallas_call(
            emit,
            out_shape=jax.ShapeDtypeStruct(shape, BF),
            in_specs=[pl.BlockSpec(memory_space=pltpu.VMEM)],
            out_specs=anywhere,
            scratch_shapes=[dma],
            name="emit",
        )(pltpu.with_memory_space_constraint(moved, pltpu.VMEM))

    return jax.shard_map(
        local,
        mesh=mesh,
        in_specs=(P("tm", "space", None, None), P("tm", "space", None, None), P(), P(), P(), P(), P(), P()),
        out_specs=P("tm", "space", None, None),
        check_vma=False,
    )
```

```python
import numpy as np
import jax
import jax.numpy as jnp
from jax import lax
from jax.experimental import pallas as pl
from jax.experimental.pallas import tpu as pltpu
from jax.sharding import PartitionSpec as P

HEADS = 8
C = 256
W = 256
FL = 4
RL = 4
BF = jnp.bfloat16
F32 = jnp.float32
MESH = pl.DeviceIdType.MESH


def tables():
    at = np.arange(256)
    col_of = (at % 16) * 16 + at // 16
    columns = np.zeros((256, 256), np.float32)
    columns[at, col_of] = 1.0
    channel = np.zeros((256, 256), np.float32)
    channel[at, (at % 32) * 8 + at // 32] = 1.0
    same = (at[:, None] // 128 == at[None, :] // 128) & (at[:, None] % 8 == at[None, :] % 8)
    heads = same.astype(np.float32)
    widen = np.zeros((256, 128), np.float32)
    for col in range(256):
        half = col // 2
        other = max(half - 1, 0) if col % 2 == 0 else min(half + 1, 127)
        widen[col, half] += 0.75
        widen[col, other] += 0.25
    widen = widen[col_of]
    none = np.zeros_like(widen)

    def pair(first, second):
        return np.concatenate([first * widen, second * widen], axis=1)

    stack = [columns, channel, channel.T, heads, pair(0.75, 0), pair(0.75, 0.25), pair(0.25, 0.75), pair(0, 0.75), pair(0.25, 0), pair(0, 0.25)]
    return np.stack(stack).astype(jnp.bfloat16)


def positions():
    half = C // 2
    inverse = np.exp(-np.log(10000.0) * 2.0 * np.arange(half) / C)
    angles = np.arange(8)[:, None] * inverse[None, :]
    return np.concatenate([np.sin(angles), np.cos(angles)], axis=1).astype(np.float32)[:, None, :]


def taps(ref, lead, first, rows):
    parts = []
    for dy in range(3):
        for dx in range(3):
            parts.append(ref[lead, first + dy : first + dy + rows, 16 * dx : 16 * dx + 256, :].reshape(rows * 256, C))
    return jnp.concatenate(parts, axis=1)


def pads(ref, lead, row):
    index = lax.broadcasted_iota(jnp.int32, (16, C), 0)
    last = ref[lead, row, 256:272, :].astype(F32)
    before = jnp.where(index == 0, 0.0, pltpu.roll(last, 1, axis=0))
    ref[lead, row, 0:16, :] = before.astype(BF)
    leading = ref[lead, row, 16:32, :].astype(F32)
    after = jnp.where(index == 15, 0.0, pltpu.roll(leading, 15, axis=0))
    ref[lead, row, 272:288, :] = after.astype(BF)


def kernel(
    spaces,
    fine_hbm, coarse_hbm, wq_hbm, wk_hbm, wv_hbm, wo_hbm, c1_hbm, c2_hbm, mats_hbm, pos_hbm,
    ob,
    fin, cb, raw, mats, pos, cw1, cw2,
    wqp, wkv, wop, nbuf, fp, qs, kb, vb, att, xp, yp, acc, psend, precv,
    load_sem, row_sem, nsend, nrecv, xsend, xrecv, tsend, trecv, near_sem, far_sem,
):
    t = lax.axis_index("tm")
    s = lax.axis_index("space")
    has_up = s > 0
    has_down = s < spaces - 1

    def rows_load(k):
        return pltpu.make_async_copy(fine_hbm.at[:, pl.ds(1, 2)], fin.at[:, pl.ds(1, 2)], row_sem.at[k])

    loads = [
        pltpu.make_async_copy(mats_hbm.at[0], mats.at[0], load_sem.at[0]),
        pltpu.make_async_copy(mats_hbm.at[pl.ds(0, 4)], raw, load_sem.at[1]),
        pltpu.make_async_copy(pos_hbm, pos, load_sem.at[2]),
        pltpu.make_async_copy(mats_hbm.at[pl.ds(1, 2)], mats.at[pl.ds(1, 2)], load_sem.at[3]),
        pltpu.make_async_copy(coarse_hbm, cb, load_sem.at[4]),
        pltpu.make_async_copy(c1_hbm, cw1, load_sem.at[5]),
        pltpu.make_async_copy(c2_hbm, cw2, load_sem.at[6]),
        pltpu.make_async_copy(mats_hbm.at[pl.ds(3, 7)], mats.at[pl.ds(3, 7)], load_sem.at[7]),
    ]
    for r in (3, 0):
        for f in range(FL):
            pltpu.make_async_copy(fine_hbm.at[f, r], fin.at[f, r], row_sem.at[0]).start()
    loads[0].start()
    loads[2].start()
    for k, weight in enumerate((wq_hbm, wk_hbm, wv_hbm, wo_hbm)):
        pltpu.make_async_copy(weight, raw.at[k], load_sem.at[1]).start()
    loads[3].start()

    barrier = pltpu.get_barrier_semaphore()

    @pl.when(t == 1)
    def _():
        pl.semaphore_signal(barrier, inc=1, device_id=(1 - t, s), device_id_type=MESH)


    @pl.when(t == 0)
    def _():
        pl.semaphore_wait(barrier, 1)
        pl.semaphore_signal(near_sem, inc=1, device_id=(1 - t, s), device_id_type=MESH)

    @pl.when(t == 1)
    def _():
        pl.semaphore_wait(near_sem, 1)

    @pl.when(jnp.logical_and(t == 1, has_up))
    def _():
        pl.semaphore_signal(barrier, inc=1, device_id=(t, s - 1), device_id_type=MESH)

    @pl.when(jnp.logical_and(t == 1, has_down))
    def _():
        pl.semaphore_signal(barrier, inc=1, device_id=(t, s + 1), device_id_type=MESH)

    zero_row = jnp.zeros((FL, 288, C), BF)

    @pl.when(jnp.logical_not(has_up))
    def _():
        xp[:, 0] = zero_row

    @pl.when(jnp.logical_not(has_down))
    def _():
        xp[:, 5] = zero_row

    def norm_copy(k):
        r = (0, 3, 0, 3, 1, 2)[k]
        px = pl.ds((0, 0, 128, 128, 0, 0)[k], 128 if k < 4 else 256)
        return pltpu.make_async_remote_copy(
            src_ref=nbuf.at[pl.ds(0, FL), r, px], dst_ref=nbuf.at[pl.ds(FL, FL), r, px],
            send_sem=nsend, recv_sem=nrecv.at[k],
            device_id=(1 - t, s), device_id_type=MESH)

    def normalize(units, start, count):
        px = slice(start, start + count)
        placed = [jnp.dot(mats[0, px], fin[f, r], preferred_element_type=F32) for f, r in units]
        for (f, r), moved in zip(units, placed):
            fp[f, r, px] = moved.astype(BF)
            hidden = moved + pos[t * FL + f]
            center = hidden - jnp.mean(hidden, axis=-1, keepdims=True)
            spread = jnp.mean(center * center, axis=-1, keepdims=True)
            nbuf[f, r, px] = (center * lax.rsqrt(spread + 1e-05)).astype(BF)

    def edge_copy(a, up, h):
        row, slot, to = (1, 5, s - 1) if up else (4, 0, s + 1)
        side = 0 if up else 1
        px = pl.ds(16 + 128 * h, 128)
        return pltpu.make_async_remote_copy(
            src_ref=xp.at[a, row, px], dst_ref=xp.at[a, slot, px],
            send_sem=xsend.at[side], recv_sem=xrecv.at[side, a],
            device_id=(t, to), device_id_type=MESH)

    def part_copy(a, up):
        side = 0 if up else 1
        to = s - 1 if up else s + 1
        return pltpu.make_async_remote_copy(
            src_ref=psend.at[side, a], dst_ref=precv.at[side, a],
            send_sem=tsend.at[side], recv_sem=trecv.at[side, a],
            device_id=(t, to), device_id_type=MESH)

    factor = float(np.log2(np.e) / np.sqrt(32.0))

    def project(rows, frames, own, start, count):
        px = slice(start, start + count)
        units = [(b, r) for b in frames for r in rows]
        stacked = jnp.concatenate([nbuf[b, r, px] for b, r in units], axis=0)
        both = jnp.dot(stacked, wkv[...], preferred_element_type=F32)
        if own:
            query = jnp.dot(stacked, wqp[...], preferred_element_type=F32)
        for i, (b, r) in enumerate(units):
            at = slice(count * i, count * i + count)
            kb[r, b, px] = both[at, 0:256].astype(BF)
            vb[r, b, px] = both[at, 256:512].astype(BF)
            if own:
                qs[r, b, px] = (query[at] * factor).astype(BF)

    def weigh(a, r, start, into):
        px = slice(start, start + 64)
        out = slice(into, into + 64)
        q = qs[r, a, px]
        lhs = []
        for pair in range(4):
            halves = []
            for b in (2 * pair, 2 * pair + 1):
                product = q * kb[r, b, px]
                halves.append(product[:, 0:128] + product[:, 128:256])
            lhs.append(jnp.concatenate(halves, axis=1))
        both = jnp.dot(jnp.concatenate(lhs, axis=0), mats[3], preferred_element_type=F32)
        scores = []
        for b in range(8):
            at = 64 * (b // 2)
            scores.append(both[at : at + 64, 128 * (b % 2) : 128 * (b % 2) + 128])
        largest = scores[0]
        for entry in scores[1:]:
            largest = jnp.maximum(largest, entry)
        powers = [jnp.exp2(entry - largest) for entry in scores]
        total = powers[0]
        for entry in powers[1:]:
            total = total + entry
        inverse = 1.0 / total
        low, high = [], []
        for b in range(8):
            weight = powers[b].astype(BF)
            value = vb[r, b, px]
            low.append(weight * value[:, 0:128])
            high.append(weight * value[:, 128:256])
        while len(low) > 1:
            low = [low[j] + low[j + 1] for j in range(0, len(low), 2)]
            high = [high[j] + high[j + 1] for j in range(0, len(high), 2)]
        att[out, 0:128] = (low[0].astype(F32) * inverse).astype(BF)
        att[out, 128:256] = (high[0].astype(F32) * inverse).astype(BF)

    def attend(units, count, beside=()):
        beside = list(beside)
        into = 0
        for a, r, start in units:
            for px in range(start, start + count, 64):
                weigh(a, r, px, into)
                into += 64
                if into % 128 == 0 and beside:
                    beside.pop(0)()
        for run in beside:
            run()
        branch = jnp.dot(att[0:into], wop[...], preferred_element_type=F32)
        for i, (a, r, start) in enumerate(units):
            px = slice(start, start + count)
            moved = (fp[a, r, px].astype(F32) + branch[count * i : count * i + count]).astype(BF)
            fp[a, r, px] = moved
            xp[a, r + 1, 16 + start : 16 + start + count, :] = jnp.maximum(moved, jnp.zeros_like(moved))

    def send_up(a, h):
        @pl.when(has_up)
        def _():
            edge_copy(a, True, h).start()

    def send_down(a, h):
        @pl.when(has_down)
        def _():
            edge_copy(a, False, h).start()

    def send_edges(a, h):
        send_down(a, h)
        send_up(a, h)

    def wait_norms(ks):
        with jax.named_scope("norm_wait"):
            for k in ks:
                norm_copy(k).wait_recv()

    def edge_whole(a, up):
        row, slot, to = (1, 5, s - 1) if up else (4, 0, s + 1)
        side = 0 if up else 1
        return pltpu.make_async_remote_copy(
            src_ref=xp.at[a, row, pl.ds(16, 256)], dst_ref=xp.at[a, slot, pl.ds(16, 256)],
            send_sem=xsend.at[side], recv_sem=xrecv.at[side, a],
            device_id=(t, to), device_id_type=MESH)

    def first_wait(a):
        @pl.when(has_up)
        def _():
            with jax.named_scope("edge_wait_up"):
                edge_whole(a, False).wait_recv()

        @pl.when(has_down)
        def _():
            with jax.named_scope("edge_wait_down"):
                edge_whole(a, True).wait_recv()

    def first_rows(a, rows):
        weight = cw1[...].reshape(9 * C, C)

        def run(y):
            result = jnp.dot(taps(xp, a, y, 1), weight, preferred_element_type=F32)
            yp[a, 1 + y, 16:272, :] = jnp.maximum(result, 0.0).astype(BF)

        return [lambda y=y: run(y) for y in rows]

    def first_end(a):
        for r in range(1, 5):
            pads(yp, a, r)
        near = cb[a].reshape(256, C)
        parts = []
        for side, row, dy in ((0, 1, 2), (1, 4, 0)):
            lhs = jnp.concatenate([yp[a, row, 16 * dx : 16 * dx + 256, :] for dx in range(3)], axis=1)
            parts.append(jnp.dot(lhs, cw2[dy].reshape(3 * C, C), preferred_element_type=F32))
        for side in (0, 1):
            parts[side] = parts[side] + jnp.dot(mats[8 + side], near, preferred_element_type=F32)
        for side in (0, 1):
            psend[side, a] = parts[side].astype(BF)

    def send_parts(a):
        @pl.when(has_up)
        def _():
            part_copy(a, True).start()

        @pl.when(has_down)
        def _():
            part_copy(a, False).start()

    with jax.named_scope("load_wait"):
        loads[0].wait()
        loads[2].wait()
        rows_load(0).wait()
    loads[7].start()
    rows_load(1).start()
    for copy in loads[4:7]:
        copy.start()
    edge_units = [(f, r) for f in range(FL) for r in (0, 3)]
    with jax.named_scope("norm03"):
        normalize(edge_units[1::2], 0, 128)
    norm_copy(1).start()
    with jax.named_scope("norm0"):
        normalize(edge_units[0::2], 0, 128)
    norm_copy(0).start()
    with jax.named_scope("weights"):
        loads[1].wait()
        loads[3].wait()
        wqp[...] = jnp.dot(raw[0], mats[1], preferred_element_type=F32).astype(BF)
        wkv[:, 0:256] = jnp.dot(raw[1], mats[1], preferred_element_type=F32).astype(BF)
        wkv[:, 256:512] = jnp.dot(raw[2], mats[1], preferred_element_type=F32).astype(BF)
        wop[...] = jnp.dot(mats[2], raw[3], preferred_element_type=F32).astype(BF)
    with jax.named_scope("keys03"):
        project((0, 3), range(0, 4), True, 0, 128)
    with jax.named_scope("norm03b"):
        normalize(edge_units, 128, 128)
    norm_copy(3).start()
    norm_copy(2).start()

    def edge_pair(k, h, beside):
        frames = (2 * k, 2 * k + 1)
        attend([(a, r, 128 * h) for a in frames for r in (0, 3)], 128, beside)
        for a in frames:
            send_edges(a, h)

    @pl.when(t == 1)
    def _():
        pl.semaphore_wait(barrier, has_up.astype(jnp.int32) + has_down.astype(jnp.int32))
        pl.semaphore_signal(far_sem, inc=1, device_id=(1 - t, s), device_id_type=MESH)

    with jax.named_scope("attend03"):
        loads[7].wait()
        wait_norms((1,))
        project((3,), range(4, 8), False, 0, 128)
        attend([(0, 3, 0)], 128)
        with jax.named_scope("meet"):
            @pl.when(t == 0)
            def _():
                pl.semaphore_wait(far_sem, 1)

        send_down(0, 0)
        wait_norms((0,))
        project((0,), range(4, 8), False, 0, 128)
        attend([(0, 0, 0)], 128)
        send_up(0, 0)
        attend([(1, 0, 0), (1, 3, 0)], 128, [lambda k=k: project((0, 3), (2 * k, 2 * k + 1), True, 128, 128) for k in range(2)])
        send_edges(1, 0)
    def inner_norm(pair, carry):
        normalize([(2 * pair + k, r) for k in range(2) for r in (1, 2)], 0, 256)
        return carry

    wait_norms((2, 3))
    with jax.named_scope("attend03b"):
        project((0, 3), range(4, 8), False, 128, 128)
        edge_pair(0, 1, [])
    with jax.named_scope("norm12"):
        rows_load(1).wait()
        lax.fori_loop(0, 2, inner_norm, 0)
    norm_copy(4).start()
    norm_copy(5).start()
    with jax.named_scope("attend03c"):
        edge_pair(1, 0, [lambda b=b: project((1, 2), (b,), True, 0, 256) for b in range(0, 4)])
    with jax.named_scope("attend03d"):
        edge_pair(1, 1, [])
    wait_norms((4, 5))
    with jax.named_scope("keys12b"):
        for b in range(4, 8, 2):
            project((1, 2), (b, b + 1), False, 0, 256)
    with jax.named_scope("attend12"):
        attend([(0, 1, 0), (0, 2, 0)], 256)
    for copy in loads[4:7]:
        copy.wait()

    def mixed_step(a, carry):
        for r in range(1, 5):
            pads(xp, a, r)
        attend([(a + 1, 1, 0), (a + 1, 2, 0)], 256, first_rows(a, (1, 2)))
        first_wait(a)
        outer(a)
        send_parts(a)
        return carry

    def outer(a):
        for r in (0, 5):
            pads(xp, a, r)
        for run in first_rows(a, (0, 3)):
            run()
        first_end(a)

    with jax.named_scope("mixed"):
        lax.fori_loop(0, FL - 1, mixed_step, 0)
    with jax.named_scope("first"):
        for r in range(1, 5):
            pads(xp, FL - 1, r)
        first_wait(FL - 1)
        outer(FL - 1)
        send_parts(FL - 1)
        for run in first_rows(FL - 1, (1, 2)):
            run()
        for r in (2, 3):
            pads(yp, FL - 1, r)

    def second_step(a, carry):
        near = cb[a].reshape(256, C)
        inner = jnp.dot(taps(yp, a, 1, 2), cw2[...].reshape(9 * C, C), preferred_element_type=F32)
        outer = []
        for row, first, dys in ((0, 1, (1, 2)), (3, 3, (0, 1))):
            parts = [yp[a, first + k, 16 * dx : 16 * dx + 256, :] for k in range(2) for dx in range(3)]
            weight = cw2[dys[0] : dys[0] + 2].reshape(6 * C, C)
            outer.append(jnp.dot(jnp.concatenate(parts, axis=1), weight, preferred_element_type=F32))
        up = jnp.dot(mats[4:8].reshape(4 * 256, 256), near, preferred_element_type=F32)
        for row, value in ((1, inner[0:256]), (2, inner[256:512]), (0, outer[0]), (3, outer[1])):
            value = value + up[256 * row : 256 * row + 256] + fp[a, row].astype(F32)
            if row in (1, 2):
                fp[a, row] = value.astype(BF)
            else:
                acc[a, row // 3] = value
        return carry

    with jax.named_scope("second"):
        lax.fori_loop(0, FL, second_step, 0)

    def edge_part(a, side):
        near = cb[a].reshape(256, C)
        precv[1 - side, a] = jnp.dot(mats[8 + side], near, preferred_element_type=F32).astype(BF)

    def last_row(a, k):
        value = (acc[a, k] + precv[1 - k, a].astype(F32)).astype(BF)
        ob[a, 3 * k] = jnp.dot(mats[0], value, preferred_element_type=F32).astype(BF)

    def last_step(a, carry):
        @pl.when(has_down)
        def _():
            with jax.named_scope("part_wait_down"):
                part_copy(a, True).wait_recv()

        @pl.when(jnp.logical_not(has_down))
        def _():
            edge_part(a, 1)

        last_row(a, 1)

        @pl.when(has_up)
        def _():
            with jax.named_scope("part_wait_up"):
                part_copy(a, False).wait_recv()

        @pl.when(jnp.logical_not(has_up))
        def _():
            edge_part(a, 0)

        last_row(a, 0)
        return carry

    def restore_step(a, carry):
        for row in (1, 2):
            ob[a, row] = jnp.dot(mats[0], fp[a, row], preferred_element_type=F32).astype(BF)
        return carry

    with jax.named_scope("restore"):
        lax.fori_loop(0, FL, restore_step, 0)
    with jax.named_scope("last"):
        lax.fori_loop(0, FL, last_step, 0)

    with jax.named_scope("drain"):
        pltpu.make_async_remote_copy(
            src_ref=nbuf.at[pl.ds(0, FL)], dst_ref=nbuf.at[pl.ds(FL, FL)], send_sem=nsend, recv_sem=nrecv.at[0],
            device_id=(1 - t, s), device_id_type=MESH).wait_send()
        for side, flag, row, slot, to in ((0, has_up, 1, 5, s - 1), (1, has_down, 4, 0, s + 1)):
            @pl.when(flag)
            def _(side=side, row=row, slot=slot, to=to):
                pltpu.make_async_remote_copy(
                    src_ref=xp.at[:, row, pl.ds(16, 256)], dst_ref=xp.at[:, slot, pl.ds(16, 256)],
                    send_sem=xsend.at[side], recv_sem=xrecv.at[side, 0],
                    device_id=(t, to), device_id_type=MESH).wait_send()
                pltpu.make_async_remote_copy(
                    src_ref=psend.at[side], dst_ref=precv.at[side],
                    send_sem=tsend.at[side], recv_sem=trecv.at[side, 0],
                    device_id=(t, to), device_id_type=MESH).wait_send()


def solution(mesh):
    spaces = mesh.shape["space"]
    constants = tables()
    place = positions()

    def local(fine, coarse, w_query, w_key, w_value, w_out, conv_first, conv_second):
        anywhere = pl.BlockSpec(memory_space=pl.ANY)
        dma = pltpu.SemaphoreType.DMA
        shape = (FL, RL, W, C)
        mats = jnp.asarray(constants)
        moved = pl.pallas_call(
            lambda *refs: kernel(spaces, *refs),
            out_shape=pltpu.VMEM(shape, BF),
            in_specs=[anywhere] * 10,
            out_specs=pl.BlockSpec(memory_space=pltpu.VMEM),
            scratch_shapes=[
                pltpu.VMEM(shape, BF),
                pltpu.VMEM((FL, 2, 128, C), BF),
                pltpu.VMEM((4, C, C), BF),
                pltpu.VMEM((10, 256, 256), BF),
                pltpu.VMEM((8, 1, C), F32),
                pltpu.VMEM((3, 3, C, C), BF),
                pltpu.VMEM((3, 3, C, C), BF),
                pltpu.VMEM((C, C), BF),
                pltpu.VMEM((C, 2 * C), BF),
                pltpu.VMEM((C, C), BF),
                pltpu.VMEM((2 * FL, RL, W, C), BF),
                pltpu.VMEM(shape, BF),
                pltpu.VMEM((RL, FL, W, C), BF),
                pltpu.VMEM((RL, 2 * FL, W, C), BF),
                pltpu.VMEM((RL, 2 * FL, W, C), BF),
                pltpu.VMEM((2 * W, C), BF),
                pltpu.VMEM((FL, RL + 2, W + 32, C), BF),
                pltpu.VMEM((FL, RL + 2, W + 32, C), BF),
                pltpu.VMEM((FL, 2, W, C), F32),
                pltpu.VMEM((2, FL, W, C), BF),
                pltpu.VMEM((2, FL, W, C), BF),
                dma((8,)),
                dma((2,)),
                dma,
                dma((6,)),
                dma((2,)),
                dma((2, FL)),
                dma((2,)),
                dma((2, FL)),
                pltpu.SemaphoreType.REGULAR,
                pltpu.SemaphoreType.REGULAR,
            ],
            compiler_params=pltpu.CompilerParams(
                collective_id=0, has_side_effects=True, vmem_limit_bytes=60 * 1024 * 1024),
            name="fused",
        )(fine, coarse, w_query, w_key, w_value, w_out, conv_first, conv_second, mats, jnp.asarray(place))
        def emit(x, o, sem):
            for f in range(FL):
                for r in range(0, RL, 2):
                    pltpu.make_async_copy(x.at[f, pl.ds(r, 2)], o.at[f, pl.ds(r, 2)], sem).start()
            pltpu.make_async_copy(x, o, sem).wait()

        return pl.pallas_call(
            emit,
            out_shape=jax.ShapeDtypeStruct(shape, BF),
            in_specs=[pl.BlockSpec(memory_space=pltpu.VMEM)],
            out_specs=anywhere,
            scratch_shapes=[dma],
            name="emit",
        )(pltpu.with_memory_space_constraint(moved, pltpu.VMEM))

    return jax.shard_map(
        local,
        mesh=mesh,
        in_specs=(P("tm", "space", None, None), P("tm", "space", None, None), P(), P(), P(), P(), P(), P()),
        out_specs=P("tm", "space", None, None),
        check_vma=False,
    )
```
